128 devices in a mesh: gx: 8 (over x, core), gy: 16 (over z, y).
Axes of the slice: x: 4, y: 4, z: 4, core: 2. Of those that a mesh axis runs over, the one named last changes fastest.
Arguments:
- samples: bfloat16 [128, 256, 32, 256], P('gx', 'gy'), may hold values from -6 to 6
- leaf_basis: bfloat16 [64, 256], replicated, may hold values from -0.375 to 0.375
- transfer: bfloat16 [5, 64, 256], replicated, may hold values from -0.5 to 0.5
- coupling: bfloat16 [5, 7, 64, 448], replicated, may hold values from -0.15625 to 0.15625
- near_tiles: bfloat16 [9, 256, 256], replicated, may hold values from -0.125 to 0.125
- codes_local: int32 [128, 256, 4, 27], P('gx', 'gy'), may hold values from 0 to 35, as said below
- counts_local: int32 [128, 256, 4], P('gx', 'gy'), may hold values from 1 to 27, as said below
- codes_upper: int32 [168, 27], replicated, may hold values from 0 to 35, as said below
- counts_upper: int32 [168], replicated, may hold values from 1 to 27, as said below
Outputs:
- response: bfloat16 [128, 256, 32, 256], P('gx', 'gy')
The draws below stay inside these ranges and needn't reach their ends.
Inputs may be any that keep to these rules, and one draw needn't show every extreme that they name: `codes_local`: entries [i, j, l, :] with i and j multiples of 2^l hold the list of the level-l cluster whose first leaf is (i, j); other entries are not read. Its first count entries are distinct codes a * 6 + b of clusters more than one step away from the target in some direction. `counts_local`: length of the list stored at the same position. `codes_upper`: row n is the list of the n-th cluster of level 4 and coarser, levels in order from 4, row-major within a level, each level with half the rows and columns of the one before and the last with 2 rows; first count entries distinct codes of clusters more than one step away from the target in some direction. `counts_upper`: length of the list of the same row.
All inputs are finite; a program needn't handle non-finite values.
Results may differ from the reference program's by a relative error of at most 0.0095.
Values may be sent and summed in bfloat16 or wider, within the bound.
No kernel may reach another device: no remote copies, remote signals or barrier semaphores. Data moves between devices by JAX's collectives and lax.ppermute only.
A program may use at most 384 MiB of HBM per device.

```python
import jax
import jax.numpy as jnp
import numpy as np
from jax import lax

LEAF = 256
R = 64
NV = 32
LOCAL = 4
LISTMAX = 27
PATCH = 16
NXL = 128
NYL = 256
UPPER = 168


def near_flags(row_bits, col_bits):
    code_ids = jnp.arange(36, dtype=jnp.int32)
    code_row = code_ids // 6
    code_col = code_ids % 6
    return (code_row >= 1 + row_bits[..., None]) & (code_row <= 3 + row_bits[..., None]) & (code_col >= 1 + col_bits[..., None]) & (code_col <= 3 + col_bits[..., None])


def draw_lists(key, row_bits, col_bits):
    full_shape = row_bits.shape + (36,)
    code_ids = jnp.arange(36, dtype=jnp.int32)
    scores = jax.random.randint(key, full_shape, 0, 2 ** 20, dtype=jnp.int32) * 64 + code_ids
    scores = jnp.where(near_flags(row_bits, col_bits), 2 ** 30 + code_ids, scores)
    ordering = jnp.argsort(scores, axis=-1, stable=True)
    return ordering[..., :LISTMAX].astype(jnp.int32)


def local_bits():
    level_scale = jnp.asarray([2 ** level_index for level_index in range(LOCAL)], jnp.int32)
    leaf_row = jnp.arange(NXL, dtype=jnp.int32)[:, None, None]
    leaf_col = jnp.arange(NYL, dtype=jnp.int32)[None, :, None]
    row_bits = jnp.broadcast_to(leaf_row // level_scale % 2, (NXL, NYL, LOCAL))
    col_bits = jnp.broadcast_to(leaf_col // level_scale % 2, (NXL, NYL, LOCAL))
    return (row_bits, col_bits)


def upper_positions():
    row_list = []
    col_list = []
    grid_rows = NXL // PATCH
    grid_cols = NYL // PATCH
    while grid_rows >= 2:
        row_list.append(np.repeat(np.arange(grid_rows), grid_cols))
        col_list.append(np.tile(np.arange(grid_cols), grid_rows))
        grid_rows = grid_rows // 2
        grid_cols = grid_cols // 2
    return (np.concatenate(row_list), np.concatenate(col_list))


def draw_codes_local(key, part):
    row_bits, col_bits = local_bits()
    return draw_lists(jax.random.fold_in(key, 11), row_bits, col_bits)


def draw_counts_local(key, part):
    heat_level = jax.random.randint(jax.random.fold_in(key, 21), (NXL // PATCH, NYL // PATCH, LOCAL), 1, 5, dtype=jnp.int32)
    heat_level = jnp.repeat(jnp.repeat(heat_level, PATCH, axis=0), PATCH, axis=1)
    base_count = jax.random.randint(jax.random.fold_in(key, 22), (NXL, NYL, LOCAL), 0, LISTMAX, dtype=jnp.int32)
    return (1 + base_count * heat_level // 4).astype(jnp.int32)


def draw_codes_upper(key, part):
    row_list, col_list = upper_positions()
    row_bits = jnp.asarray(row_list % 2, jnp.int32)
    col_bits = jnp.asarray(col_list % 2, jnp.int32)
    return draw_lists(jax.random.fold_in(key, 31), row_bits, col_bits)


def draw_counts_upper(key, part):
    heat_level = jax.random.randint(jax.random.fold_in(key, 41), (UPPER,), 1, 5, dtype=jnp.int32)
    base_count = jax.random.randint(jax.random.fold_in(key, 42), (UPPER,), 0, LISTMAX, dtype=jnp.int32)
    return (1 + base_count * heat_level // 4).astype(jnp.int32)


def shard_levels(own_key, extent, shards, least, high):
    loudness, own = 1.0, jax.random.fold_in(own_key, 6)
    for position, shards_of in shards:
        steps = jnp.exp(jax.random.uniform(jax.random.fold_in(own, position), (shards_of,), jnp.float32, least / len(shards), high / len(shards)))
        loudness = loudness * jnp.repeat(steps, extent[position] // shards_of).reshape([-1 if axis == position else 1 for axis in range(len(extent))])
    return loudness


def gaussian(own_key, extent, width, most, pieces=(), kind=jnp.bfloat16):
    gain = shard_levels(own_key, extent, pieces, -0.22, 0.18) if pieces else 1.0
    values = jax.random.normal(own_key, extent, jnp.float32) * width * gain
    return jnp.minimum(jnp.maximum(values, -most), most).astype(kind)


def setup_inputs(seed: int = 0) -> dict:
    splits = jax.random.split(jax.random.key(seed), 10)
    samples = gaussian(splits[0], (NXL, NYL, NV, LEAF), 1.0, 6.0, ((0, 8), (1, 16)))
    leaf_basis = gaussian(splits[1], (R, LEAF), LEAF ** -0.5, 0.375)
    transfer = gaussian(splits[2], (LOCAL + 1, R, 4 * R), (2 * R) ** -0.5, 0.5)
    coupling = gaussian(splits[3], (LOCAL + 1, 7, R, 7 * R), (27 * R) ** -0.5, 0.15625)
    near_tiles = gaussian(splits[4], (9, LEAF, LEAF), (9 * LEAF) ** -0.5, 0.125)
    codes_local = draw_codes_local(jax.random.fold_in(splits[9], 71), 0)
    counts_local = draw_counts_local(jax.random.fold_in(splits[9], 71), 0)
    codes_upper = draw_codes_upper(jax.random.fold_in(splits[9], 71), 0)
    counts_upper = draw_counts_upper(jax.random.fold_in(splits[9], 71), 0)
    return dict(samples=samples, leaf_basis=leaf_basis, transfer=transfer, coupling=coupling, near_tiles=near_tiles, codes_local=codes_local, counts_local=counts_local, codes_upper=codes_upper, counts_upper=counts_upper)


def is_near(row_step, col_step):
    return abs(row_step) <= 1 and abs(col_step) <= 1


def lift_level(children, matrices):
    grid_rows, grid_cols, vectors, rank_size = children.shape
    grouped = children.reshape(grid_rows // 2, 2, grid_cols // 2, 2, vectors, rank_size)
    grouped = grouped.transpose(0, 2, 4, 1, 3, 5).reshape(grid_rows // 2, grid_cols // 2, vectors, 4 * rank_size)
    parent = jnp.einsum('pqvc,sc->pqvs', grouped.astype(jnp.float32), matrices.astype(jnp.float32))
    return parent.astype(jnp.bfloat16)


def spread(parent, matrices):
    grid_rows, grid_cols, vectors, rank_size = parent.shape
    carried = jnp.einsum('pqvs,sc->pqvc', parent.astype(jnp.float32), matrices.astype(jnp.float32))
    carried = carried.reshape(grid_rows, grid_cols, vectors, 2, 2, rank_size).transpose(0, 3, 1, 4, 2, 5)
    return carried.reshape(2 * grid_rows, 2 * grid_cols, vectors, rank_size)


def member_table(list_codes, counts):
    slot_index = jnp.arange(list_codes.shape[-1], dtype=jnp.int32)
    active = slot_index < counts[..., None]
    matches = (list_codes[..., None] == jnp.arange(36, dtype=jnp.int32)) & active[..., None]
    return jnp.any(matches, axis=-2).astype(jnp.float32)


def couple(padded, member, matrices):
    grid_rows = padded.shape[0] - 4
    grid_cols = padded.shape[1] - 4
    vectors = padded.shape[2]
    rank_size = padded.shape[3]
    member = member.reshape(grid_rows // 2, 2, grid_cols // 2, 2, 36)
    totals = [[jnp.zeros((grid_rows // 2, grid_cols // 2, vectors, rank_size), jnp.float32) for col_bit in range(2)] for row_bit in range(2)]
    for code_row in range(6):
        for code_col in range(6):
            parities = [(row_bit, col_bit) for row_bit in range(2) for col_bit in range(2) if not is_near(code_row - 2 - row_bit, code_col - 2 - col_bit)]
            if not parities:
                continue
            source = padded[code_row:code_row + grid_rows:2, code_col:code_col + grid_cols:2]
            blocks = jnp.concatenate([matrices[code_row + 1 - row_bit, :, (code_col + 1 - col_bit) * rank_size:(code_col + 2 - col_bit) * rank_size] for (row_bit, col_bit) in parities], axis=0)
            images = jnp.einsum('pqvr,sr->pqvs', source.astype(jnp.float32), blocks.astype(jnp.float32))
            for number, (row_bit, col_bit) in enumerate(parities):
                weight_mask = member[:, row_bit, :, col_bit, code_row * 6 + code_col]
                totals[row_bit][col_bit] = totals[row_bit][col_bit] + weight_mask[..., None, None] * images[..., number * rank_size:(number + 1) * rank_size]
    stacked = jnp.stack([jnp.stack(totals[row_bit], axis=0) for row_bit in range(2)], axis=0)
    return stacked.transpose(2, 0, 3, 1, 4, 5).reshape(grid_rows, grid_cols, vectors, rank_size)


def reference(samples, leaf_basis, transfer, coupling, near_tiles, codes_local, counts_local, codes_upper, counts_upper):
    leaf_rows = samples.shape[0]
    leaf_cols = samples.shape[1]
    row_blocks = leaf_rows // PATCH
    blocked = samples.reshape(row_blocks, PATCH, leaf_cols, NV, LEAF)

    def project(rows_block):
        return jnp.einsum('ijvs,rs->ijvr', rows_block.astype(jnp.float32), leaf_basis.astype(jnp.float32)).astype(jnp.bfloat16)

    level_coeffs = [lax.map(project, blocked).reshape(leaf_rows, leaf_cols, NV, R)]
    while level_coeffs[-1].shape[0] > 2:
        level_index = len(level_coeffs) - 1
        level_coeffs.append(lift_level(level_coeffs[-1], transfer[min(level_index, LOCAL)]))

    members = []
    offset = 0
    for level_index, coeffs in enumerate(level_coeffs):
        if level_index < LOCAL:
            stride = 2 ** level_index
            members.append(member_table(codes_local[::stride, ::stride, level_index], counts_local[::stride, ::stride, level_index]))
        else:
            grid_rows = coeffs.shape[0]
            grid_cols = coeffs.shape[1]
            count_here = grid_rows * grid_cols
            members.append(member_table(codes_upper[offset:offset + count_here].reshape(grid_rows, grid_cols, LISTMAX), counts_upper[offset:offset + count_here].reshape(grid_rows, grid_cols)))
            offset = offset + count_here

    images = []
    for level_index, coeffs in enumerate(level_coeffs):
        padded = jnp.pad(coeffs, ((2, 2), (2, 2), (0, 0), (0, 0)))
        images.append(couple(padded, members[level_index], coupling[min(level_index, LOCAL)]))
    downward = images[-1]
    for level_index in range(len(level_coeffs) - 2, -1, -1):
        downward = images[level_index] + spread(downward.astype(jnp.bfloat16), transfer[min(level_index, LOCAL)])

    padded_samples = jnp.pad(samples, ((1, 1), (1, 1), (0, 0), (0, 0)))
    far_coeffs = downward.astype(jnp.bfloat16).reshape(row_blocks, PATCH, leaf_cols, NV, R)

    def finish(inputs):
        block_index, coeffs = inputs
        window = lax.dynamic_slice_in_dim(padded_samples, block_index * PATCH, PATCH + 2, 0)
        summed = jnp.einsum('ijvr,rs->ijvs', coeffs.astype(jnp.float32), leaf_basis.astype(jnp.float32))
        for step_row in range(3):
            for step_col in range(3):
                neighbour = window[step_row:step_row + PATCH, step_col:step_col + leaf_cols]
                summed = summed + jnp.einsum('ijvs,ts->ijvt', neighbour.astype(jnp.float32), near_tiles[step_row * 3 + step_col].astype(jnp.float32))
        return summed.astype(jnp.bfloat16)

    result = lax.map(finish, (jnp.arange(row_blocks, dtype=jnp.int32), far_coeffs))
    return result.reshape(leaf_rows, leaf_cols, NV, LEAF)
```

```python
import jax
import jax.numpy as jnp
from jax import lax
from jax.experimental import pallas as pl
from jax.experimental.pallas import tpu as pltpu
from jax.sharding import PartitionSpec as P


BF = jnp.bfloat16
F32 = jnp.float32
RANK = 64
VEC = 32
VMEM = pltpu.VMEM


def dot_nt(a, b):
    return lax.dot_general(a, b, (((1,), (1,)), ((), ())), preferred_element_type=F32)


def dot_nn(a, b):
    return lax.dot_general(a, b, (((1,), (0,)), ((), ())), preferred_element_type=F32)


def pair_rhs(matrix):
    zeros = jnp.zeros_like(matrix)
    return jnp.concatenate(
        [jnp.concatenate([matrix, zeros], 0), jnp.concatenate([zeros, matrix], 0)], 1
    )


def split_pairs(value):
    n, vec, k = value.shape
    v = value.reshape(n // 2, 2, vec, k)
    return jnp.concatenate(
        [v[:, 0].reshape(n // 2 * vec, k), v[:, 1].reshape(n // 2 * vec, k)], 1
    )


def lift_rows(upper, lower, rhs):
    both = jnp.concatenate([upper, lower], 2)
    out = dot_nt(split_pairs(both), rhs)
    return out.astype(BF).reshape(upper.shape[0] // 2, VEC, 128)


EDGE = 10


def gx_units(q_sizes, patch):
    def edge(last):
        units = []
        for level, n in enumerate(q_sizes):
            for row in range(2):
                units.append(("q", level, row, (n // 2 - 1) if last else 0))
        for half in range(2):
            units.append(("s", patch - 1 if last else 0, half))
        return units

    left, right = edge(False), edge(True)
    middle = []
    for level, n in enumerate(q_sizes):
        for row in range(2):
            for p in range(1, n // 2 - 1):
                middle.append(("q", level, row, p))
    for cell in range(1, patch - 1):
        for half in range(2):
            middle.append(("s", cell, half))
    return left + middle + right


def gy_starts(q_sizes, patch):
    starts = []
    at = 0
    for n in q_sizes:
        starts.append(at)
        at += n
    return starts, at, at + 2 * patch


def project_kernel(hbm_ref, basis_ref, transfer_ref, *refs):
    outs, bufs, (s_ref, sems, row_sems, out_sems) = refs[:9], refs[9:18], refs[18:]
    q0, q1, q2, q3, q4, gx_lo, gx_hi, gy_left, gy_right = bufs
    patch = s_ref.shape[0]
    qs = [q0, q1, q2, q3]
    sizes = [q.shape[0] for q in qs]

    def copy(i):
        return pltpu.make_async_copy(hbm_ref.at[i], s_ref.at[i], sems.at[i])

    def put_row(i):
        return pltpu.make_async_copy(q0.at[i], outs[0].at[i], row_sems.at[i])

    def put(k):
        return pltpu.make_async_copy(bufs[k], outs[k], out_sems.at[k])

    def fetch(i, carry):
        copy(i).start()
        return carry

    lax.fori_loop(0, patch, fetch, 0)
    basis = pair_rhs(basis_ref[...])
    starts, base, _ = gy_starts(sizes, patch)

    def row(i, carry):
        copy(i).wait()
        q0[i] = dot_nt(split_pairs(s_ref[i]), basis).astype(BF).reshape(patch // 2, VEC, 128)
        put_row(i).start()
        for half in range(2):
            cols = slice(half * 128, half * 128 + 128)
            gy_left[EDGE + base + 2 * i + half] = s_ref[i, 0, :, cols]
            gy_right[EDGE + base + 2 * i + half] = s_ref[i, patch - 1, :, cols]
        return carry

    lax.fori_loop(0, patch, row, 0)
    for level in range(3):
        rhs = pair_rhs(transfer_ref[level])
        for r in range(sizes[level + 1]):
            qs[level + 1][r] = lift_rows(qs[level][2 * r], qs[level][2 * r + 1], rhs)
        put(level + 1).start()
    for number, unit in enumerate(gx_units(sizes, patch)):
        if unit[0] == "q":
            _, level, r, p = unit
            gx_lo[number] = qs[level][r, p]
            gx_hi[number] = qs[level][sizes[level] - 2 + r, p]
        else:
            _, cell, half = unit
            gx_lo[number] = s_ref[0, cell, :, half * 128 : half * 128 + 128]
            gx_hi[number] = s_ref[patch - 1, cell, :, half * 128 : half * 128 + 128]
    put(5).start()
    put(6).start()
    both = jnp.concatenate([q3[0, 0], q3[1, 0]], 1)
    both = jnp.concatenate([both[: VEC // 2], both[VEC // 2 :]], 1)
    top = dot_nt(both, pair_rhs(transfer_ref[3])).astype(BF)
    q4[...] = jnp.broadcast_to(top[None], q4.shape)
    put(4).start()
    zeros = jnp.zeros((EDGE, VEC, 128), BF)
    for ref in (gy_left, gy_right):
        ref[0:EDGE] = zeros
        ref[ref.shape[0] - EDGE : ref.shape[0]] = zeros
    for level in range(4):
        n = sizes[level]
        at = EDGE + starts[level]
        gy_left[at : at + n] = qs[level][:, 0]
        gy_right[at : at + n] = qs[level][:, n // 2 - 1]
    put(7).start()
    put(8).start()

    def wait_row(i, carry):
        put_row(i).wait()
        return carry

    lax.fori_loop(0, patch, wait_row, 0)
    for k in range(1, 9):
        put(k).wait()


def corner_kernel(from_lo, from_hi, left_in, right_in, left, right, buf, sems):
    del left_in, right_in
    n = left.shape[0]
    m = from_lo.shape[0]
    moves = [
        (from_lo.at[0:EDGE], left.at[0:EDGE]),
        (from_hi.at[0:EDGE], left.at[n - EDGE : n]),
        (from_lo.at[m - EDGE : m], right.at[0:EDGE]),
        (from_hi.at[m - EDGE : m], right.at[n - EDGE : n]),
    ]
    gets = [pltpu.make_async_copy(a, buf.at[k], sems.at[k]) for k, (a, b) in enumerate(moves)]
    puts = [pltpu.make_async_copy(buf.at[k], b, sems.at[4 + k]) for k, (a, b) in enumerate(moves)]
    for get in gets:
        get.start()
    for get, put in zip(gets, puts):
        get.wait()
        put.start()
    for put in puts:
        put.wait()


def list_words(codes, counts):
    slot = lax.broadcasted_iota(jnp.int32, codes.shape, codes.ndim - 1)
    active = slot < counts
    words = []
    for group in range(2):
        here = active & ((codes >= 18) if group else (codes < 18))
        shift = jnp.where(here, codes - 18 * group, 0)
        power = jnp.where(here, lax.shift_left(jnp.ones_like(codes), shift), 0)
        words.append(power.astype(F32))
    return words


def word_offsets(sizes):
    offsets = [0]
    for n in sizes:
        offsets.append(offsets[-1] + n * n)
    return offsets


def near_kernel(
    s_hbm, tiles_hbm, codes_ref, counts_ref, acc_hbm, words_hbm,
    s_ref, acc_ref, w_ref, tiles_ref, words_ref, in_sems, out_sems, more_sems,
):
    patch = s_ref.shape[0]

    def fetch(i):
        return pltpu.make_async_copy(s_hbm.at[i], s_ref.at[i], in_sems.at[i])

    def put_out(k):
        rows = pl.ds(2 * k, 2)
        return pltpu.make_async_copy(acc_ref.at[rows], acc_hbm.at[rows], out_sems.at[k])

    def start_fetch(i, carry):
        fetch(i).start()
        return carry

    fetch_tiles = pltpu.make_async_copy(tiles_hbm, tiles_ref, more_sems.at[0])
    put_words = pltpu.make_async_copy(words_ref, words_hbm, more_sems.at[1])
    fetch_tiles.start()
    lax.fori_loop(0, patch, start_fetch, 0)
    levels = counts_ref.shape[1]
    at = 0
    for level in range(levels):
        n = patch >> level
        counts = counts_ref[:, level : level + 1]
        codes = codes_ref[:, level, :]
        for group, power in enumerate(list_words(codes, counts)):
            word = jnp.sum(power, axis=1, keepdims=True).astype(jnp.int32)
            word = jnp.broadcast_to(word, (patch * patch, 128))
            for i in range(n):
                for j in range(n):
                    r = ((i * patch + j) << level)
                    words_ref[at + i * n + j, group] = jnp.broadcast_to(word[r : r + 1], (8, 128))
        at += n * n
    put_words.start()
    fetch_tiles.wait()
    for k in range(9):
        w_ref[k * 256 : k * 256 + 256] = tiles_ref[k].T
    zeros = jnp.zeros((VEC, 256), BF)

    def shifted(value):
        return [
            jnp.concatenate([zeros, value[:-VEC]], 0),
            value,
            jnp.concatenate([value[VEC:], zeros], 0),
        ]

    def put(i, rows):
        blocks = [
            jnp.zeros((patch * VEC, 256), BF) if r is None else s_ref[r].reshape(patch * VEC, 256)
            for r in rows
        ]
        lhs = []
        for d in range(3):
            for upper, lower in zip(shifted(blocks[d]), shifted(blocks[d + 1])):
                lhs.append(jnp.concatenate([upper, lower], 0))
        out = dot_nn(jnp.concatenate(lhs, 1), w_ref[...])
        acc_ref[pl.ds(i, 2)] = out.reshape(2, patch, VEC, 256)

    for i in range(3):
        fetch(i).wait()
    put(0, [None, 0, 1, 2])
    put_out(0).start()

    def row(k, carry):
        i = 2 * k
        fetch(i + 1).wait()
        fetch(i + 2).wait()
        put(i, [i - 1, i, i + 1, i + 2])
        put_out(k).start()
        return carry

    lax.fori_loop(1, patch // 2 - 1, row, 0)
    fetch(patch - 1).wait()
    put(patch - 2, [patch - 3, patch - 2, patch - 1, None])
    put_out(patch // 2 - 1).start()

    def wait_out(k, carry):
        put_out(k).wait()
        return carry

    lax.fori_loop(0, patch // 2, wait_out, 0)
    put_words.wait()


def chunk_list(row_bit):
    chunks = []
    for a in range(6):
        for bp in range(3):
            if bp == 1 and 1 + row_bit <= a <= 3 + row_bit:
                continue
            chunks.append((a, bp))
    return chunks


def lane_bits():
    lane = lax.broadcasted_iota(jnp.int32, (8, 128), 1)
    return (lane >= 64).astype(jnp.int32)


def mask_of(words, a, bp, lanes):
    code = (a % 3) * 6 + 2 * bp
    bit = lax.shift_right_logical(words[a // 3], lanes + code) & 1
    m = bit.astype(F32)
    return jnp.concatenate([m, m, m, m], 0).astype(BF)


def final_kernel(
    counts_upper_ref, codes_upper_ref,
    *refs,
):
    n_in = 15
    sources, out_ref, buffers, rest = refs[:n_in], refs[n_in], refs[n_in + 1 : 2 * n_in + 1], refs[2 * n_in + 1 :]
    (
        transfer_ref, every, coupling_ref, words_ref, q0, q1, q2, q3,
        from_lo, from_hi, from_left, from_right, basis_ref, tiles_ref, acc_ref,
    ) = buffers
    (
    e0, e1, e2, e3, f4, f5, f6, shifted, b0, b1, b2, b3, cols, edge_col, edge_row, out_buf, sems, in_sems, acc_sems,
    ) = rest
    patch = acc_ref.shape[0]

    def fetch(k):
        return pltpu.make_async_copy(sources[k], buffers[k], in_sems.at[k])

    def fetch_acc(i):
        return pltpu.make_async_copy(sources[n_in - 1].at[i], acc_ref.at[i], acc_sems.at[i])

    for k in range(n_in - 1):
        fetch(k).start()

    def start_acc(i, carry):
        fetch_acc(i).start()
        return carry

    lax.fori_loop(0, patch, start_acc, 0)
    qs = [q0, q1, q2, q3]
    es = [e0, e1, e2, e3]
    sizes = [q.shape[0] for q in qs]
    lanes = lane_bits()
    word_at = word_offsets(sizes)

    for k in range(3):
        fetch(k).wait()
    for level in range(5):
        for d in range(7):
            shifted[level, d] = coupling_ref[level, d, :, 64:448]

    def block(level, col_bit, d, bp):
        if col_bit == 1:
            return coupling_ref[level, d, :, bp * 128 : bp * 128 + 128]
        return shifted[level, d, :, bp * 128 : bp * 128 + 128]

    f4[...] = jnp.zeros_like(f4)
    f5[...] = jnp.zeros_like(f5)
    f6[...] = jnp.zeros_like(f6)
    rows4 = f4.shape[0] - 4
    pairs4 = f4.shape[1] - 2
    low = lax.broadcasted_iota(jnp.int32, (pairs4, VEC // 2, 128), 2) < 64
    for r in range(rows4):
        v = every[2 * pairs4 * r : 2 * pairs4 * (r + 1)].astype(F32).reshape(pairs4, 2, VEC // 2, 128)
        even, odd = v[:, 0], v[:, 1]
        top = jnp.where(low, even, pltpu.roll(odd, 64, 2))
        bottom = jnp.where(low, pltpu.roll(even, 64, 2), odd)
        f4[r + 2, 1 : pairs4 + 1] = jnp.concatenate([top, bottom], 1).astype(BF)
    rhs4 = pair_rhs(transfer_ref[4])
    for child, parent in ((f4, f5), (f5, f6)):
        n_rows = parent.shape[0] - 4
        n_pairs = child.shape[1] - 2
        for r in range(n_rows):
            parent[r + 2, 1 : n_pairs // 2 + 1] = lift_rows(
                child[2 * r + 2, 1 : n_pairs + 1], child[2 * r + 3, 1 : n_pairs + 1], rhs4
            )
    row_index = lax.axis_index("gx")
    col_index = lax.axis_index("gy")
    upper_codes = codes_upper_ref[...]
    upper_slot = lax.broadcasted_iota(jnp.int32, upper_codes.shape, 0)
    upper_list = lax.broadcasted_iota(jnp.int32, upper_codes.shape, 1)

    def upper_words(index):
        count = jnp.where(upper_list == index, counts_upper_ref[index], 0)
        here = upper_slot < count
        words = []
        for group in range(2):
            mine = here & ((upper_codes >= 18) if group else (upper_codes < 18))
            shift = jnp.where(mine, upper_codes - 18 * group, 0)
            power = jnp.where(mine, lax.shift_left(jnp.ones_like(shift), shift), 0)
            total = jnp.sum(power.astype(F32), axis=0, keepdims=True)
            total = jnp.sum(total, axis=1, keepdims=True)
            words.append(jnp.broadcast_to(total, (8, 128)).astype(jnp.int32))
        return words

    uppers = []
    offset = 0
    for step, f in enumerate((f4, f5, f6)):
        r_here = lax.shift_right_logical(row_index, step)
        c_here = lax.shift_right_logical(col_index, step)
        n_cols = 2 * (f.shape[1] - 2)
        index = offset + r_here * n_cols + c_here
        offset += (f.shape[0] - 4) * n_cols
        words = upper_words(index)
        rb = r_here & 1
        cb = c_here & 1
        top_row = r_here - rb
        left = lax.shift_right_logical(c_here, 1)
        lhs, rhs = [], []
        for a in range(6):
            for bp in range(3):
                lhs.append(f[top_row + a, left + bp] * mask_of(words, a, bp, lanes))
            even = shifted[4, a + 1 - rb]
            odd = coupling_ref[4, a + 1 - rb][:, 0:384]
            rhs.append(jnp.where(cb == 1, odd, even))
        uppers.append(dot_nt(jnp.concatenate(lhs, 1), jnp.concatenate(rhs, 1)))
    down = uppers[-1]
    for step in (1, 0):
        r_here = lax.shift_right_logical(row_index, step)
        c_here = lax.shift_right_logical(col_index, step)
        carried = dot_nn(down.astype(BF), transfer_ref[4])
        half = jnp.where((r_here & 1) == 1, carried[:, 128:256], carried[:, 0:128])
        half = jnp.where((c_here & 1) == 1, pltpu.roll(half, 64, 1), half)
        down = uppers[step] + half[:, 0:64]
    carried3 = dot_nn(down.astype(BF), transfer_ref[3])

    for k in range(3, 12):
        fetch(k).wait()
    for level in range(4):
        n = sizes[level]
        es[level][2 : n + 2, 1 : n // 2 + 1] = qs[level][...]
    row_cells = {}
    for number, unit in enumerate(gx_units(sizes, patch)):
        if unit[0] == "q":
            _, level, r, p = unit
            es[level][r, p + 1] = from_lo[number]
            es[level][sizes[level] + 2 + r, p + 1] = from_hi[number]
        else:
            row_cells[unit[1:]] = number
    starts, base, total = gy_starts(sizes, patch)
    for side, ref in ((0, from_left), (1, from_right)):
        for level in range(4):
            n = sizes[level]
            p = 0 if side == 0 else n // 2 + 1
            es[level][0:2, p] = ref[2 * level : 2 * level + 2]
            es[level][2 : n + 2, p] = ref[EDGE + starts[level] : EDGE + starts[level] + n]
            hi = EDGE + total
            es[level][n + 2 : n + 4, p] = ref[hi + 2 * level : hi + 2 * level + 2]
        for half in range(2):
            c = slice(half * 128, half * 128 + 128)
            cols[side, 0, :, c] = ref[8 + half]
            cols[side, patch + 1, :, c] = ref[EDGE + total + 8 + half]
            for i in range(patch):
                cols[side, i + 1, :, c] = ref[EDGE + base + 2 * i + half]

    def images(level, group_rows, row_bit):
        n = sizes[level]
        e = es[level]
        out = []
        for col_bit in range(2):
            lhs, rhs = [], []
            words = []
            for group_row in group_rows:
                for group_col in range(n // 2):
                    at = word_at[level] + (2 * group_row + row_bit) * n + 2 * group_col + col_bit
                    words.append((words_ref[at, 0], words_ref[at, 1]))
            for a, bp in chunk_list(row_bit):
                rows = []
                for number, pair in enumerate(words):
                    group_row = group_rows[number // (n // 2)]
                    group_col = number % (n // 2)
                    rows.append(
                        e[2 * group_row + a, group_col + bp] * mask_of(pair, a, bp, lanes)
                    )
                lhs.append(jnp.concatenate(rows, 0))
                rhs.append(block(level, col_bit, a + 1 - row_bit, bp))
            out.append(dot_nt(jnp.concatenate(lhs, 1), jnp.concatenate(rhs, 1)))
        return jnp.concatenate(out, 1)

    def spread_rhs(level):
        t = transfer_ref[level]
        z = jnp.zeros_like(t)
        return [jnp.concatenate([t, z], 0), jnp.concatenate([z, t], 0)]

    for row_bit in range(2):
        u = images(3, [0], row_bit)
        b3[row_bit, 0] = (u + carried3[:, row_bit * 128 : row_bit * 128 + 128]).astype(BF)

    def descend(level, parent, child, group_rows):
        n_pairs = parent.shape[1]
        count = len(group_rows)
        value = jnp.concatenate([parent[r].reshape(n_pairs * VEC, 128) for r in group_rows], 0)
        even, odd = [
            dot_nn(value, rhs).reshape(count, n_pairs, 1, VEC, 256) for rhs in spread_rhs(level)
        ]
        carried = jnp.concatenate([even, odd], 2).reshape(count, 2 * n_pairs, VEC, 256)
        for row_bit in range(2):
            u = images(level, group_rows, row_bit).reshape(count, 2 * n_pairs, VEC, 128)
            u = u + carried[:, :, :, row_bit * 128 : row_bit * 128 + 128]
            for number, group_row in enumerate(group_rows):
                child[2 * group_row + row_bit] = u[number].astype(BF)

    descend(2, b3, b2, [0, 1])
    descend(1, b2, b1, list(range(sizes[1] // 2)))

    def loop0(k, carry):
        descend(0, b1, b0, [2 * k, 2 * k + 1])
        return carry

    lax.fori_loop(0, sizes[0] // 4, loop0, 0)

    for k in range(12, n_in - 1):
        fetch(k).wait()
    for side in range(2):
        lhs = jnp.concatenate(
            [cols[side, d : d + patch].reshape(patch * VEC, 256) for d in range(3)], 1
        )
        rhs = jnp.concatenate([tiles_ref[3 * d + 2 * side] for d in range(3)], 1)
        edge_col[side] = dot_nt(lhs, rhs).reshape(patch, VEC, 256)
    for side, ref in ((0, from_lo), (1, from_hi)):
        cells = [
            jnp.concatenate([ref[row_cells[(j, half)]] for half in range(2)], 1)
            for j in range(patch)
        ]
        zeros = jnp.zeros((VEC, 256), BF)
        lhs = jnp.concatenate(
            [
                jnp.concatenate([zeros] + cells[:-1], 0),
                jnp.concatenate(cells, 0),
                jnp.concatenate(cells[1:] + [zeros], 0),
            ],
            1,
        )
        rhs = jnp.concatenate([tiles_ref[6 * side + d] for d in range(3)], 1)
        edge_row[side] = dot_nt(lhs, rhs).reshape(patch, VEC, 256)

    basis = basis_ref[...]
    zb = jnp.zeros_like(basis)
    basis_pair = [jnp.concatenate([basis, zb], 0), jnp.concatenate([zb, basis], 0)]

    def copy(i):
        return pltpu.make_async_copy(out_buf.at[i], out_ref.at[i], sems.at[i])

    def finish(i, extra):
        fetch_acc(i).wait()
        value = b0[i].reshape(patch // 2 * VEC, 128)
        far = [dot_nn(value, rhs).reshape(patch // 2, 1, VEC, 256) for rhs in basis_pair]
        total_row = jnp.concatenate(far, 1).reshape(patch, VEC, 256) + acc_ref[i]
        if extra is not None:
            total_row = total_row + edge_row[extra]
        first = total_row[0:1] + edge_col[0, pl.ds(i, 1)]
        last = total_row[patch - 1 : patch] + edge_col[1, pl.ds(i, 1)]
        total_row = jnp.concatenate([first, total_row[1 : patch - 1], last], 0)
        out_buf[i] = total_row.astype(BF)
        copy(i).start()

    finish(0, 0)
    finish(patch - 1, 1)

    def loop_out(i, carry):
        finish(i, None)
        return carry

    lax.fori_loop(1, patch - 1, loop_out, 0)

    def loop_wait(i, carry):
        copy(i).wait()
        return carry

    lax.fori_loop(0, patch, loop_wait, 0)


def vspec():
    return pl.BlockSpec(memory_space=VMEM)


def sspec():
    return pl.BlockSpec(memory_space=pltpu.SMEM)


def shards(
    samples, leaf_basis, transfer, coupling, near_tiles,
    codes_local, counts_local, codes_upper, counts_upper,
):
    patch = samples.shape[0]
    sizes = [patch // 2**k for k in range(4)]
    n_gx = lax.axis_size("gx")
    n_gy = lax.axis_size("gy")
    units_gx = len(gx_units(sizes, patch))
    units_gy = gy_starts(sizes, patch)[2]
    params = pltpu.CompilerParams(vmem_limit_bytes=56 * 1024 * 1024)

    anywhere = pl.BlockSpec(memory_space=pl.ANY)
    shapes = [(n, n // 2, VEC, 128) for n in sizes]
    shapes += [(n_gx * n_gy, VEC // 2, 128)]
    shapes += [(units_gx, VEC, 128)] * 2 + [(units_gy + 2 * EDGE, VEC, 128)] * 2
    outs = pl.pallas_call(
        project_kernel,
        out_shape=[jax.ShapeDtypeStruct(v, BF) for v in shapes],
        in_specs=[anywhere, vspec(), vspec()],
        out_specs=[anywhere] * 9,
        scratch_shapes=[pltpu.VMEM(v, BF) for v in shapes]
        + [
            pltpu.VMEM((patch, patch, VEC, 256), BF),
            pltpu.SemaphoreType.DMA((patch,)),
            pltpu.SemaphoreType.DMA((patch,)),
            pltpu.SemaphoreType.DMA((9,)),
        ],
        compiler_params=params,
        name="project",
    )(samples, leaf_basis, transfer)
    q0, q1, q2, q3, q4, gx_lo, gx_hi, gy_left, gy_right = outs

    up = lambda n: [(i, i + 1) for i in range(n - 1)]
    dn = lambda n: [(i + 1, i) for i in range(n - 1)]
    from_lo = lax.ppermute(gx_hi, "gx", up(n_gx))
    from_hi = lax.ppermute(gx_lo, "gx", dn(n_gx))
    every = lax.all_to_all(q4, ("gx", "gy"), 0, 0, tiled=True)
    full = jax.ShapeDtypeStruct((units_gy + 2 * EDGE, VEC, 128), BF)
    send_left, send_right = pl.pallas_call(
        corner_kernel,
        out_shape=[full, full],
        in_specs=[anywhere] * 4,
        out_specs=[anywhere] * 2,
        scratch_shapes=[pltpu.VMEM((4, EDGE, VEC, 128), BF), pltpu.SemaphoreType.DMA((8,))],
        input_output_aliases={2: 0, 3: 1},
        compiler_params=params,
        name="corner",
    )(from_lo, from_hi, gy_left, gy_right)
    from_left = lax.ppermute(send_right, "gy", up(n_gy))
    from_right = lax.ppermute(send_left, "gy", dn(n_gy))

    n_words = word_offsets(sizes)[-1]
    acc, words = pl.pallas_call(
        near_kernel,
        out_shape=[
            jax.ShapeDtypeStruct((patch, patch, VEC, 256), F32),
            jax.ShapeDtypeStruct((n_words, 2, 8, 128), jnp.int32),
        ],
        in_specs=[anywhere, anywhere, vspec(), vspec()],
        out_specs=[anywhere, anywhere],
        scratch_shapes=[
            pltpu.VMEM((patch, patch, VEC, 256), BF),
            pltpu.VMEM((patch, patch, VEC, 256), F32),
            pltpu.VMEM((9 * 256, 256), BF),
            pltpu.VMEM(near_tiles.shape, BF),
            pltpu.VMEM((n_words, 2, 8, 128), jnp.int32),
            pltpu.SemaphoreType.DMA((patch,)),
            pltpu.SemaphoreType.DMA((patch // 2,)),
            pltpu.SemaphoreType.DMA((2,)),
        ],
        compiler_params=params,
        name="near",
    )(
        samples, near_tiles,
        codes_local.reshape(patch * patch, *codes_local.shape[2:]),
        counts_local.reshape(patch * patch, counts_local.shape[2]),
    )

    def padded(rows, pairs):
        return pltpu.VMEM((rows + 4, pairs + 2, VEC, 128), BF)

    inputs = [
        transfer, every, coupling, words, q0, q1, q2, q3,
        from_lo, from_hi, from_left, from_right, leaf_basis, near_tiles, acc,
    ]
    scratch = [pltpu.VMEM(v.shape, v.dtype) for v in inputs]
    scratch += [padded(n, n // 2) for n in sizes]
    scratch += [padded(n_gx // 2**k, n_gy // 2 ** (k + 1)) for k in range(3)]
    scratch += [pltpu.VMEM((5, 7, RANK, 384), BF)]
    scratch += [pltpu.VMEM((n, n // 2, VEC, 128), BF) for n in sizes]
    scratch += [
        pltpu.VMEM((2, patch + 2, VEC, 256), BF),
        pltpu.VMEM((2, patch, VEC, 256), F32),
        pltpu.VMEM((2, patch, VEC, 256), F32),
        pltpu.VMEM((patch, patch, VEC, 256), BF),
        pltpu.SemaphoreType.DMA((patch,)),
        pltpu.SemaphoreType.DMA((len(inputs) - 1,)),
        pltpu.SemaphoreType.DMA((patch,)),
    ]
    return pl.pallas_call(
        final_kernel,
        out_shape=jax.ShapeDtypeStruct((patch, patch, VEC, 256), BF),
        in_specs=[sspec(), vspec()] + [anywhere] * len(inputs),
        out_specs=pl.BlockSpec(memory_space=pl.ANY),
        scratch_shapes=scratch,
        compiler_params=params,
        name="final",
    )(
        counts_upper, codes_upper.T, *inputs,
    )


def solution(mesh):
    big = P("gx", "gy", None, None)
    in_specs = (big, P(), P(), P(), P(), big, P("gx", "gy", None), P(), P())
    return jax.shard_map(shards, mesh=mesh, in_specs=in_specs, out_specs=big, check_vma=False)
```

```python
import jax
import jax.numpy as jnp
from jax import lax
from jax.experimental import pallas as pl
from jax.experimental.pallas import tpu as pltpu
from jax.sharding import PartitionSpec as P


BF = jnp.bfloat16
F32 = jnp.float32
RANK = 64
VEC = 32
VMEM = pltpu.VMEM


def dot_nt(a, b):
    return lax.dot_general(a, b, (((1,), (1,)), ((), ())), preferred_element_type=F32)


def dot_nn(a, b):
    return lax.dot_general(a, b, (((1,), (0,)), ((), ())), preferred_element_type=F32)


def pair_rhs(matrix):
    zeros = jnp.zeros_like(matrix)
    return jnp.concatenate(
        [jnp.concatenate([matrix, zeros], 0), jnp.concatenate([zeros, matrix], 0)], 1
    )


def split_pairs(value):
    n, vec, k = value.shape
    v = value.reshape(n // 2, 2, vec, k)
    return jnp.concatenate(
        [v[:, 0].reshape(n // 2 * vec, k), v[:, 1].reshape(n // 2 * vec, k)], 1
    )


def lift_rows(upper, lower, rhs):
    both = jnp.concatenate([upper, lower], 2)
    out = dot_nt(split_pairs(both), rhs)
    return out.astype(BF).reshape(upper.shape[0] // 2, VEC, 128)


EDGE = 10


def gx_units(q_sizes, patch):
    def edge(last):
        units = []
        for level, n in enumerate(q_sizes):
            for row in range(2):
                units.append(("q", level, row, (n // 2 - 1) if last else 0))
        for half in range(2):
            units.append(("s", patch - 1 if last else 0, half))
        return units

    left, right = edge(False), edge(True)
    middle = []
    for level, n in enumerate(q_sizes):
        for row in range(2):
            for p in range(1, n // 2 - 1):
                middle.append(("q", level, row, p))
    for cell in range(1, patch - 1):
        for half in range(2):
            middle.append(("s", cell, half))
    return left + middle + right


def gy_starts(q_sizes, patch):
    starts = []
    at = 0
    for n in q_sizes:
        starts.append(at)
        at += n
    return starts, at, at + 2 * patch


def project_kernel(hbm_ref, basis_hbm, transfer_hbm, *refs):
    outs, bufs = refs[:9], refs[9:18]
    s_ref, basis_ref, transfer_ref, sems, row_sems, out_sems, more_sems = refs[18:]
    q0, q1, q2, q3, q4, gx_lo, gx_hi, gy_left, gy_right = bufs
    patch = s_ref.shape[0]
    qs = [q0, q1, q2, q3]
    sizes = [q.shape[0] for q in qs]

    def copy(i):
        return pltpu.make_async_copy(hbm_ref.at[i], s_ref.at[i], sems.at[i])

    def put_row(i):
        return pltpu.make_async_copy(q0.at[i], outs[0].at[i], row_sems.at[i])

    def put(k):
        return pltpu.make_async_copy(bufs[k], outs[k], out_sems.at[k])

    def fetch(i, carry):
        copy(i).start()
        return carry

    get_basis = pltpu.make_async_copy(basis_hbm, basis_ref, more_sems.at[0])
    get_transfer = pltpu.make_async_copy(transfer_hbm, transfer_ref, more_sems.at[1])
    get_basis.start()
    lax.fori_loop(0, patch, fetch, 0)
    get_transfer.start()
    get_basis.wait()
    basis = pair_rhs(basis_ref[...])
    starts, base, _ = gy_starts(sizes, patch)

    def row(i, carry):
        copy(i).wait()
        q0[i] = dot_nt(split_pairs(s_ref[i]), basis).astype(BF).reshape(patch // 2, VEC, 128)
        put_row(i).start()
        for half in range(2):
            cols = slice(half * 128, half * 128 + 128)
            gy_left[EDGE + base + 2 * i + half] = s_ref[i, 0, :, cols]
            gy_right[EDGE + base + 2 * i + half] = s_ref[i, patch - 1, :, cols]
        return carry

    lax.fori_loop(0, patch, row, 0)
    get_transfer.wait()
    for level in range(3):
        rhs = pair_rhs(transfer_ref[level])
        for r in range(sizes[level + 1]):
            qs[level + 1][r] = lift_rows(qs[level][2 * r], qs[level][2 * r + 1], rhs)
        put(level + 1).start()
    for number, unit in enumerate(gx_units(sizes, patch)):
        if unit[0] == "q":
            _, level, r, p = unit
            gx_lo[number] = qs[level][r, p]
            gx_hi[number] = qs[level][sizes[level] - 2 + r, p]
        else:
            _, cell, half = unit
            gx_lo[number] = s_ref[0, cell, :, half * 128 : half * 128 + 128]
            gx_hi[number] = s_ref[patch - 1, cell, :, half * 128 : half * 128 + 128]
    put(5).start()
    put(6).start()
    both = jnp.concatenate([q3[0, 0], q3[1, 0]], 1)
    both = jnp.concatenate([both[: VEC // 2], both[VEC // 2 :]], 1)
    top = dot_nt(both, pair_rhs(transfer_ref[3])).astype(BF)
    q4[...] = jnp.broadcast_to(top[None], q4.shape)
    put(4).start()
    zeros = jnp.zeros((EDGE, VEC, 128), BF)
    for ref in (gy_left, gy_right):
        ref[0:EDGE] = zeros
        ref[ref.shape[0] - EDGE : ref.shape[0]] = zeros
    for level in range(4):
        n = sizes[level]
        at = EDGE + starts[level]
        gy_left[at : at + n] = qs[level][:, 0]
        gy_right[at : at + n] = qs[level][:, n // 2 - 1]
    put(7).start()
    put(8).start()

    def wait_row(i, carry):
        put_row(i).wait()
        return carry

    lax.fori_loop(0, patch, wait_row, 0)
    for k in range(1, 9):
        put(k).wait()


def corner_kernel(from_lo, from_hi, left_in, right_in, left, right, buf, sems):
    del left_in, right_in
    n = left.shape[0]
    m = from_lo.shape[0]
    moves = [
        (from_lo.at[0:EDGE], left.at[0:EDGE]),
        (from_hi.at[0:EDGE], left.at[n - EDGE : n]),
        (from_lo.at[m - EDGE : m], right.at[0:EDGE]),
        (from_hi.at[m - EDGE : m], right.at[n - EDGE : n]),
    ]
    gets = [pltpu.make_async_copy(a, buf.at[k], sems.at[k]) for k, (a, b) in enumerate(moves)]
    puts = [pltpu.make_async_copy(buf.at[k], b, sems.at[4 + k]) for k, (a, b) in enumerate(moves)]
    for get in gets:
        get.start()
    for get, put in zip(gets, puts):
        get.wait()
        put.start()
    for put in puts:
        put.wait()


def list_words(codes, counts):
    slot = lax.broadcasted_iota(jnp.int32, codes.shape, codes.ndim - 1)
    active = slot < counts
    words = []
    for group in range(2):
        here = active & ((codes >= 18) if group else (codes < 18))
        shift = jnp.where(here, codes - 18 * group, 0)
        power = jnp.where(here, lax.shift_left(jnp.ones_like(codes), shift), 0)
        words.append(power.astype(F32))
    return words


def half_sizes(patch):
    return [patch // 2**k for k in range(4)]


def word_offsets(sizes):
    offsets = [0]
    for n in sizes:
        offsets.append(offsets[-1] + n * n)
    return offsets


def near_kernel(
    s_hbm, tiles_hbm, codes_hbm, counts_hbm, lo_hbm, hi_hbm, acc_hbm, words_hbm,
    s_ref, acc_ref, w_ref, tiles_ref, words_ref, codes_ref, counts_ref, lo_ref, hi_ref,
    in_sems, out_sems, more_sems,
):
    patch = s_ref.shape[0]

    def fetch(i):
        return pltpu.make_async_copy(s_hbm.at[i], s_ref.at[i], in_sems.at[i])

    def put_out(k):
        rows = pl.ds(2 * k, 2)
        return pltpu.make_async_copy(acc_ref.at[rows], acc_hbm.at[rows], out_sems.at[k])

    def start_fetch(i, carry):
        fetch(i).start()
        return carry

    pairs = [(codes_hbm, codes_ref), (counts_hbm, counts_ref), (lo_hbm, lo_ref), (hi_hbm, hi_ref)]
    more = [pltpu.make_async_copy(a, b, more_sems.at[2 + k]) for k, (a, b) in enumerate(pairs)]
    for copy in more:
        copy.start()
    fetch_tiles = pltpu.make_async_copy(tiles_hbm, tiles_ref, more_sems.at[0])
    put_words = pltpu.make_async_copy(words_ref, words_hbm, more_sems.at[1])
    fetch_tiles.start()
    lax.fori_loop(0, patch, start_fetch, 0)
    for copy in more:
        copy.wait()
    levels = counts_ref.shape[1]
    at = 0
    for level in range(levels):
        n = patch >> level
        counts = counts_ref[:, level : level + 1]
        codes = codes_ref[:, level, :]
        for group, power in enumerate(list_words(codes, counts)):
            word = jnp.sum(power, axis=1, keepdims=True).astype(jnp.int32)
            word = jnp.broadcast_to(word, (patch * patch, 128))
            if level == 0:
                words_ref[group, 0 : n * n] = word
                continue
            for i in range(n):
                for j in range(n):
                    r = (i * patch + j) << level
                    k = at + i * n + j
                    words_ref[group, k : k + 1] = word[r : r + 1]
        at += n * n
    put_words.start()
    fetch_tiles.wait()
    for k in range(9):
        w_ref[k * 256 : k * 256 + 256] = tiles_ref[k].T
    zeros = jnp.zeros((VEC, 256), BF)

    def shifted(value):
        return [
            jnp.concatenate([zeros, value[:-VEC]], 0),
            value,
            jnp.concatenate([value[VEC:], zeros], 0),
        ]

    def put(i, rows):
        blocks = [
            r if getattr(r, "ndim", 0) == 2 else s_ref[r].reshape(patch * VEC, 256) for r in rows
        ]
        lhs = []
        for d in range(3):
            for upper, lower in zip(shifted(blocks[d]), shifted(blocks[d + 1])):
                lhs.append(jnp.concatenate([upper, lower], 0))
        out = dot_nn(jnp.concatenate(lhs, 1), w_ref[...])
        acc_ref[pl.ds(i, 2)] = out.reshape(2, patch, VEC, 256)

    for i in range(3):
        fetch(i).wait()
    cells = {unit[1:]: k for k, unit in enumerate(gx_units(half_sizes(patch), patch)) if unit[0] == "s"}

    def halo_row(ref):
        return jnp.concatenate(
            [
                jnp.concatenate([ref[cells[(j, half)]] for j in range(patch)], 0)
                for half in range(2)
            ],
            1,
        )

    put(0, [halo_row(lo_ref), 0, 1, 2])
    put_out(0).start()

    def row(k, carry):
        i = 2 * k
        fetch(i + 1).wait()
        fetch(i + 2).wait()
        put(i, [i - 1, i, i + 1, i + 2])
        put_out(k).start()
        return carry

    lax.fori_loop(1, patch // 2 - 1, row, 0)
    fetch(patch - 1).wait()
    put(patch - 2, [patch - 3, patch - 2, patch - 1, halo_row(hi_ref)])
    put_out(patch // 2 - 1).start()

    def wait_out(k, carry):
        put_out(k).wait()
        return carry

    lax.fori_loop(0, patch // 2, wait_out, 0)
    put_words.wait()


def chunk_list(row_bit):
    chunks = []
    for a in range(6):
        for bp in range(3):
            if bp == 1 and 1 + row_bit <= a <= 3 + row_bit:
                continue
            chunks.append((a, bp))
    return chunks


def lane_bits():
    lane = lax.broadcasted_iota(jnp.int32, (8, 128), 1)
    return (lane >= 64).astype(jnp.int32)


def mask_of(words, a, bp, lanes):
    code = (a % 3) * 6 + 2 * bp
    bit = lax.shift_right_logical(words[a // 3], lanes + code) & 1
    m = bit.astype(F32)
    return jnp.concatenate([m, m, m, m], 0).astype(BF)


def upper_kernel(
    counts_upper_ref, codes_upper_ref, every_hbm, transfer_hbm, coupling_hbm, out_ref,
    every, transfer_ref, coupling_ref, shifted, f4, f5, f6, sems,
):
    pairs = [(every_hbm, every), (transfer_hbm, transfer_ref)]
    pairs += [(coupling_hbm.at[coupling_hbm.shape[0] - 1], coupling_ref)]
    copies = [pltpu.make_async_copy(a, b, sems.at[k]) for k, (a, b) in enumerate(pairs)]
    for copy in copies:
        copy.start()
    lanes = lane_bits()
    for copy in copies:
        copy.wait()
    for d in range(7):
        shifted[d] = coupling_ref[d, :, 64:448]

    f4[...] = jnp.zeros_like(f4)
    f5[...] = jnp.zeros_like(f5)
    f6[...] = jnp.zeros_like(f6)
    rows4 = f4.shape[0] - 4
    pairs4 = f4.shape[1] - 2
    low = lax.broadcasted_iota(jnp.int32, (pairs4, VEC // 2, 128), 2) < 64
    for r in range(rows4):
        v = every[2 * pairs4 * r : 2 * pairs4 * (r + 1)].astype(F32).reshape(pairs4, 2, VEC // 2, 128)
        even, odd = v[:, 0], v[:, 1]
        top = jnp.where(low, even, pltpu.roll(odd, 64, 2))
        bottom = jnp.where(low, pltpu.roll(even, 64, 2), odd)
        f4[r + 2, 1 : pairs4 + 1] = jnp.concatenate([top, bottom], 1).astype(BF)
    rhs4 = pair_rhs(transfer_ref[4])
    for child, parent in ((f4, f5), (f5, f6)):
        n_rows = parent.shape[0] - 4
        n_pairs = child.shape[1] - 2
        for r in range(n_rows):
            parent[r + 2, 1 : n_pairs // 2 + 1] = lift_rows(
                child[2 * r + 2, 1 : n_pairs + 1], child[2 * r + 3, 1 : n_pairs + 1], rhs4
            )
    row_index = lax.axis_index("gx")
    col_index = lax.axis_index("gy")
    upper_codes = codes_upper_ref[...]
    upper_slot = lax.broadcasted_iota(jnp.int32, upper_codes.shape, 0)
    upper_list = lax.broadcasted_iota(jnp.int32, upper_codes.shape, 1)

    def upper_words(index):
        count = jnp.where(upper_list == index, counts_upper_ref[index], 0)
        here = upper_slot < count
        words = []
        for group in range(2):
            mine = here & ((upper_codes >= 18) if group else (upper_codes < 18))
            shift = jnp.where(mine, upper_codes - 18 * group, 0)
            power = jnp.where(mine, lax.shift_left(jnp.ones_like(shift), shift), 0)
            total = jnp.sum(power.astype(F32), axis=0, keepdims=True)
            total = jnp.sum(total, axis=1, keepdims=True)
            words.append(jnp.broadcast_to(total, (8, 128)).astype(jnp.int32))
        return words

    uppers = []
    offset = 0
    for step, f in enumerate((f4, f5, f6)):
        r_here = lax.shift_right_logical(row_index, step)
        c_here = lax.shift_right_logical(col_index, step)
        n_cols = 2 * (f.shape[1] - 2)
        index = offset + r_here * n_cols + c_here
        offset += (f.shape[0] - 4) * n_cols
        words = upper_words(index)
        rb = r_here & 1
        cb = c_here & 1
        top_row = r_here - rb
        left = lax.shift_right_logical(c_here, 1)
        lhs, rhs = [], []
        for a in range(6):
            for bp in range(3):
                lhs.append(f[top_row + a, left + bp] * mask_of(words, a, bp, lanes))
            even = shifted[a + 1 - rb]
            odd = coupling_ref[a + 1 - rb][:, 0:384]
            rhs.append(jnp.where(cb == 1, odd, even))
        uppers.append(dot_nt(jnp.concatenate(lhs, 1), jnp.concatenate(rhs, 1)))
    down = uppers[-1]
    for step in (1, 0):
        r_here = lax.shift_right_logical(row_index, step)
        c_here = lax.shift_right_logical(col_index, step)
        carried = dot_nn(down.astype(BF), transfer_ref[4])
        half = jnp.where((r_here & 1) == 1, carried[:, 128:256], carried[:, 0:128])
        half = jnp.where((c_here & 1) == 1, pltpu.roll(half, 64, 1), half)
        down = uppers[step] + half[:, 0:64]
    out_ref[...] = dot_nn(down.astype(BF), transfer_ref[3])


def final_kernel(
    *refs,
):
    n_in = 14
    sources, coupling_hbm, out_ref = refs[:n_in], refs[n_in], refs[n_in + 1]
    buffers, rest = refs[n_in + 2 : 2 * n_in + 2], refs[2 * n_in + 2 :]
    (
        transfer_ref, carried_ref, words_ref, q0, q1, q2, q3,
        from_lo, from_hi, from_left, from_right, basis_ref, tiles_ref, acc_ref,
    ) = buffers
    (
    e0, e1, e2, e3, shifted, b0, b1, b2, b3, cols, edge_col, out_buf, coupling_ref,
    sems, in_sems, acc_sems, level_sems,
    ) = rest
    patch = acc_ref.shape[0]

    def fetch(k):
        return pltpu.make_async_copy(sources[k], buffers[k], in_sems.at[k])

    def fetch_acc(i):
        return pltpu.make_async_copy(sources[n_in - 1].at[i], acc_ref.at[i], acc_sems.at[i])

    def fetch_level(level):
        return pltpu.make_async_copy(
            coupling_hbm.at[level], coupling_ref.at[level], level_sems.at[level]
        )

    for k in range(11):
        fetch(k).start()
    for level in (3, 2, 1, 0):
        fetch_level(level).start()
    for k in range(11, n_in - 1):
        fetch(k).start()

    def start_acc(i, carry):
        fetch_acc(i).start()
        return carry

    qs = [q0, q1, q2, q3]
    es = [e0, e1, e2, e3]
    sizes = [q.shape[0] for q in qs]
    lanes = lane_bits()
    word_at = word_offsets(sizes)

    def get_level(level):
        fetch_level(level).wait()
        for d in range(7):
            shifted[level, d] = coupling_ref[level, d, :, 64:448]

    def block(level, col_bit, d, bp):
        if col_bit == 1:
            return coupling_ref[level, d, :, bp * 128 : bp * 128 + 128]
        return shifted[level, d, :, bp * 128 : bp * 128 + 128]

    for k in range(11):
        fetch(k).wait()
    for level in range(4):
        n = sizes[level]
        es[level][2 : n + 2, 1 : n // 2 + 1] = qs[level][...]
    for number, unit in enumerate(gx_units(sizes, patch)):
        if unit[0] == "q":
            _, level, r, p = unit
            es[level][r, p + 1] = from_lo[number]
            es[level][sizes[level] + 2 + r, p + 1] = from_hi[number]
    starts, base, total = gy_starts(sizes, patch)
    for side, ref in ((0, from_left), (1, from_right)):
        for level in range(4):
            n = sizes[level]
            p = 0 if side == 0 else n // 2 + 1
            es[level][0:2, p] = ref[2 * level : 2 * level + 2]
            es[level][2 : n + 2, p] = ref[EDGE + starts[level] : EDGE + starts[level] + n]
            hi = EDGE + total
            es[level][n + 2 : n + 4, p] = ref[hi + 2 * level : hi + 2 * level + 2]
        for half in range(2):
            c = slice(half * 128, half * 128 + 128)
            cols[side, 0, :, c] = ref[8 + half]
            cols[side, patch + 1, :, c] = ref[EDGE + total + 8 + half]
            for i in range(patch):
                cols[side, i + 1, :, c] = ref[EDGE + base + 2 * i + half]

    def images(level, group_rows, row_bit):
        n = sizes[level]
        e = es[level]
        out = []
        for col_bit in range(2):
            lhs, rhs = [], []
            words = []
            for group_row in group_rows:
                for group_col in range(n // 2):
                    at = word_at[level] + (2 * group_row + row_bit) * n + 2 * group_col + col_bit
                    words.append(
                        [
                            jnp.broadcast_to(words_ref[g, pl.ds(at, 1)], (8, 128))
                            for g in range(2)
                        ]
                    )
            for a, bp in chunk_list(row_bit):
                rows = []
                for number, pair in enumerate(words):
                    group_row = group_rows[number // (n // 2)]
                    group_col = number % (n // 2)
                    rows.append(
                        e[2 * group_row + a, group_col + bp] * mask_of(pair, a, bp, lanes)
                    )
                lhs.append(jnp.concatenate(rows, 0))
                rhs.append(block(level, col_bit, a + 1 - row_bit, bp))
            out.append(dot_nt(jnp.concatenate(lhs, 1), jnp.concatenate(rhs, 1)))
        return jnp.concatenate(out, 1)

    def spread_rhs(level):
        t = transfer_ref[level]
        z = jnp.zeros_like(t)
        return [jnp.concatenate([t, z], 0), jnp.concatenate([z, t], 0)]

    lax.fori_loop(0, patch, start_acc, 0)
    for level in (3, 2, 1, 0):
        get_level(level)
    carried3 = carried_ref[...]
    for row_bit in range(2):
        u = images(3, [0], row_bit)
        b3[row_bit, 0] = (u + carried3[:, row_bit * 128 : row_bit * 128 + 128]).astype(BF)

    def descend(level, parent, child, group_rows):
        n_pairs = parent.shape[1]
        count = len(group_rows)
        value = jnp.concatenate([parent[r].reshape(n_pairs * VEC, 128) for r in group_rows], 0)
        even, odd = [
            dot_nn(value, rhs).reshape(count, n_pairs, 1, VEC, 256) for rhs in spread_rhs(level)
        ]
        carried = jnp.concatenate([even, odd], 2).reshape(count, 2 * n_pairs, VEC, 256)
        for row_bit in range(2):
            u = images(level, group_rows, row_bit).reshape(count, 2 * n_pairs, VEC, 128)
            u = u + carried[:, :, :, row_bit * 128 : row_bit * 128 + 128]
            for number, group_row in enumerate(group_rows):
                child[2 * group_row + row_bit] = u[number].astype(BF)

    descend(2, b3, b2, [0, 1])
    descend(1, b2, b1, list(range(sizes[1] // 2)))

    def loop0(k, carry):
        descend(0, b1, b0, [2 * k, 2 * k + 1])
        return carry

    lax.fori_loop(0, sizes[0] // 4, loop0, 0)

    for k in range(11, n_in - 1):
        fetch(k).wait()
    for side in range(2):
        lhs = jnp.concatenate(
            [cols[side, d : d + patch].reshape(patch * VEC, 256) for d in range(3)], 1
        )
        rhs = jnp.concatenate([tiles_ref[3 * d + 2 * side] for d in range(3)], 1)
        edge_col[side] = dot_nt(lhs, rhs).reshape(patch, VEC, 256)
    basis = basis_ref[...]
    zb = jnp.zeros_like(basis)
    basis_pair = [jnp.concatenate([basis, zb], 0), jnp.concatenate([zb, basis], 0)]

    def copy(i):
        return pltpu.make_async_copy(out_buf.at[i], out_ref.at[i], sems.at[i])

    def finish(i, carry):
        fetch_acc(i).wait()
        value = b0[i].reshape(patch // 2 * VEC, 128)
        far = [dot_nn(value, rhs).reshape(patch // 2, 1, VEC, 256) for rhs in basis_pair]
        total_row = jnp.concatenate(far, 1).reshape(patch, VEC, 256) + acc_ref[i]
        first = total_row[0:1] + edge_col[0, pl.ds(i, 1)]
        last = total_row[patch - 1 : patch] + edge_col[1, pl.ds(i, 1)]
        total_row = jnp.concatenate([first, total_row[1 : patch - 1], last], 0)
        out_buf[i] = total_row.astype(BF)
        copy(i).start()
        return carry

    lax.fori_loop(0, patch, finish, 0)

    def loop_wait(i, carry):
        copy(i).wait()
        return carry

    lax.fori_loop(0, patch, loop_wait, 0)


def vspec():
    return pl.BlockSpec(memory_space=VMEM)


def sspec():
    return pl.BlockSpec(memory_space=pltpu.SMEM)


def shards(
    samples, leaf_basis, transfer, coupling, near_tiles,
    codes_local, counts_local, codes_upper, counts_upper,
):
    patch = samples.shape[0]
    sizes = [patch // 2**k for k in range(4)]
    n_gx = lax.axis_size("gx")
    n_gy = lax.axis_size("gy")
    units_gx = len(gx_units(sizes, patch))
    units_gy = gy_starts(sizes, patch)[2]
    params = pltpu.CompilerParams(vmem_limit_bytes=56 * 1024 * 1024)

    anywhere = pl.BlockSpec(memory_space=pl.ANY)
    shapes = [(n, n // 2, VEC, 128) for n in sizes]
    shapes += [(n_gx * n_gy, VEC // 2, 128)]
    shapes += [(units_gx, VEC, 128)] * 2 + [(units_gy + 2 * EDGE, VEC, 128)] * 2
    outs = pl.pallas_call(
        project_kernel,
        out_shape=[jax.ShapeDtypeStruct(v, BF) for v in shapes],
        in_specs=[anywhere] * 3,
        out_specs=[anywhere] * 9,
        scratch_shapes=[pltpu.VMEM(v, BF) for v in shapes]
        + [
            pltpu.VMEM((patch, patch, VEC, 256), BF),
            pltpu.VMEM(leaf_basis.shape, BF),
            pltpu.VMEM(transfer.shape, BF),
            pltpu.SemaphoreType.DMA((patch,)),
            pltpu.SemaphoreType.DMA((patch,)),
            pltpu.SemaphoreType.DMA((9,)),
            pltpu.SemaphoreType.DMA((2,)),
        ],
        compiler_params=params,
        name="project",
    )(samples, leaf_basis, transfer)
    q0, q1, q2, q3, q4, gx_lo, gx_hi, gy_left, gy_right = outs

    up = lambda n: [(i, i + 1) for i in range(n - 1)]
    dn = lambda n: [(i + 1, i) for i in range(n - 1)]
    from_lo = lax.ppermute(gx_hi, "gx", up(n_gx))
    from_hi = lax.ppermute(gx_lo, "gx", dn(n_gx))
    every = lax.all_to_all(q4, ("gx", "gy"), 0, 0, tiled=True)
    full = jax.ShapeDtypeStruct((units_gy + 2 * EDGE, VEC, 128), BF)
    send_left, send_right = pl.pallas_call(
        corner_kernel,
        out_shape=[full, full],
        in_specs=[anywhere] * 4,
        out_specs=[anywhere] * 2,
        scratch_shapes=[pltpu.VMEM((4, EDGE, VEC, 128), BF), pltpu.SemaphoreType.DMA((8,))],
        input_output_aliases={2: 0, 3: 1},
        compiler_params=params,
        name="corner",
    )(from_lo, from_hi, gy_left, gy_right)
    from_left = lax.ppermute(send_right, "gy", up(n_gy))
    from_right = lax.ppermute(send_left, "gy", dn(n_gy))

    n_words = -(-word_offsets(sizes)[-1] // 8) * 8
    codes = codes_local.reshape(patch * patch, *codes_local.shape[2:])
    counts = counts_local.reshape(patch * patch, counts_local.shape[2])
    acc, words = pl.pallas_call(
        near_kernel,
        out_shape=[
            jax.ShapeDtypeStruct((patch, patch, VEC, 256), F32),
            jax.ShapeDtypeStruct((2, n_words, 128), jnp.int32),
        ],
        in_specs=[anywhere] * 6,
        out_specs=[anywhere, anywhere],
        scratch_shapes=[
            pltpu.VMEM((patch, patch, VEC, 256), BF),
            pltpu.VMEM((patch, patch, VEC, 256), F32),
            pltpu.VMEM((9 * 256, 256), BF),
            pltpu.VMEM(near_tiles.shape, BF),
            pltpu.VMEM((2, n_words, 128), jnp.int32),
            pltpu.VMEM(codes.shape, codes.dtype),
            pltpu.VMEM(counts.shape, counts.dtype),
            pltpu.VMEM(from_lo.shape, BF),
            pltpu.VMEM(from_hi.shape, BF),
            pltpu.SemaphoreType.DMA((patch,)),
            pltpu.SemaphoreType.DMA((patch // 2,)),
            pltpu.SemaphoreType.DMA((6,)),
        ],
        compiler_params=params,
        name="near",
    )(
        samples, near_tiles, codes, counts, from_lo, from_hi,
    )

    def padded(rows, pairs):
        return pltpu.VMEM((rows + 4, pairs + 2, VEC, 128), BF)

    carried = pl.pallas_call(
        upper_kernel,
        out_shape=jax.ShapeDtypeStruct((VEC, transfer.shape[2]), F32),
        in_specs=[sspec(), vspec()] + [anywhere] * 3,
        out_specs=vspec(),
        scratch_shapes=[
            pltpu.VMEM(every.shape, BF),
            pltpu.VMEM(transfer.shape, BF),
            pltpu.VMEM(coupling.shape[1:], BF),
            pltpu.VMEM((7, RANK, 384), BF),
        ]
        + [padded(n_gx // 2**k, n_gy // 2 ** (k + 1)) for k in range(3)]
        + [pltpu.SemaphoreType.DMA((3,))],
        compiler_params=params,
        name="upper",
    )(counts_upper, codes_upper.T, every, transfer, coupling)
    inputs = [
        transfer, carried, words, q0, q1, q2, q3,
        from_lo, from_hi, from_left, from_right, leaf_basis, near_tiles, acc,
    ]
    scratch = [pltpu.VMEM(v.shape, v.dtype) for v in inputs]
    scratch += [padded(n, n // 2) for n in sizes]
    scratch += [pltpu.VMEM((4, 7, RANK, 384), BF)]
    scratch += [pltpu.VMEM((n, n // 2, VEC, 128), BF) for n in sizes]
    scratch += [
        pltpu.VMEM((2, patch + 2, VEC, 256), BF),
        pltpu.VMEM((2, patch, VEC, 256), F32),
        pltpu.VMEM((patch, patch, VEC, 256), BF),
        pltpu.VMEM((4, *coupling.shape[1:]), BF),
        pltpu.SemaphoreType.DMA((patch,)),
        pltpu.SemaphoreType.DMA((len(inputs) - 1,)),
        pltpu.SemaphoreType.DMA((patch,)),
        pltpu.SemaphoreType.DMA((4,)),
    ]
    return pl.pallas_call(
        final_kernel,
        out_shape=jax.ShapeDtypeStruct((patch, patch, VEC, 256), BF),
        in_specs=[anywhere] * (len(inputs) + 1),
        out_specs=pl.BlockSpec(memory_space=pl.ANY),
        scratch_shapes=scratch,
        compiler_params=params,
        name="final",
    )(
        *inputs, coupling,
    )


def solution(mesh):
    big = P("gx", "gy", None, None)
    in_specs = (big, P(), P(), P(), P(), big, P("gx", "gy", None), P(), P())
    return jax.shard_map(shards, mesh=mesh, in_specs=in_specs, out_specs=big, check_vma=False)
```

```python
import jax
import jax.numpy as jnp
from jax import lax
from jax.experimental import pallas as pl
from jax.experimental.pallas import tpu as pltpu
from jax.sharding import PartitionSpec as P


BF = jnp.bfloat16
F32 = jnp.float32
RANK = 64
VEC = 32
VMEM = pltpu.VMEM


def dot_nt(a, b):
    return lax.dot_general(a, b, (((1,), (1,)), ((), ())), preferred_element_type=F32)


def dot_nn(a, b):
    return lax.dot_general(a, b, (((1,), (0,)), ((), ())), preferred_element_type=F32)


def pair_rhs(matrix):
    zeros = jnp.zeros_like(matrix)
    return jnp.concatenate(
        [jnp.concatenate([matrix, zeros], 0), jnp.concatenate([zeros, matrix], 0)], 1
    )


def split_pairs(value):
    n, vec, k = value.shape
    v = value.reshape(n // 2, 2, vec, k)
    return jnp.concatenate(
        [v[:, 0].reshape(n // 2 * vec, k), v[:, 1].reshape(n // 2 * vec, k)], 1
    )


def lift_rows(upper, lower, rhs):
    both = jnp.concatenate([upper, lower], 2)
    out = dot_nt(split_pairs(both), rhs)
    return out.astype(BF).reshape(upper.shape[0] // 2, VEC, 128)


EDGE = 10


def gx_units(q_sizes, patch):
    def edge(last):
        units = []
        for level, n in enumerate(q_sizes):
            for row in range(2):
                units.append(("q", level, row, (n // 2 - 1) if last else 0))
        for half in range(2):
            units.append(("s", patch - 1 if last else 0, half))
        return units

    left, right = edge(False), edge(True)
    middle = []
    for level, n in enumerate(q_sizes):
        for row in range(2):
            for p in range(1, n // 2 - 1):
                middle.append(("q", level, row, p))
    for cell in range(1, patch - 1):
        for half in range(2):
            middle.append(("s", cell, half))
    return left + middle + right


def gy_starts(q_sizes, patch):
    starts = []
    at = 0
    for n in q_sizes:
        starts.append(at)
        at += n
    return starts, at, at + 2 * patch


def project_kernel(hbm_ref, basis_hbm, transfer_hbm, *refs):
    outs, bufs = refs[:9], refs[9:18]
    s_ref, basis_ref, transfer_ref, sems, row_sems, out_sems, more_sems = refs[18:]
    q0, q1, q2, q3, q4, gx_lo, gx_hi, gy_left, gy_right = bufs
    patch = s_ref.shape[0]
    qs = [q0, q1, q2, q3]
    sizes = [q.shape[0] for q in qs]

    def copy(i):
        return pltpu.make_async_copy(hbm_ref.at[i], s_ref.at[i], sems.at[i])

    def put_row(i):
        return pltpu.make_async_copy(q0.at[i], outs[0].at[i], row_sems.at[i])

    def put(k):
        return pltpu.make_async_copy(bufs[k], outs[k], out_sems.at[k])

    def fetch(i, carry):
        copy(i).start()
        return carry

    get_basis = pltpu.make_async_copy(basis_hbm, basis_ref, more_sems.at[0])
    get_transfer = pltpu.make_async_copy(transfer_hbm, transfer_ref, more_sems.at[1])
    get_basis.start()
    lax.fori_loop(0, patch, fetch, 0)
    get_transfer.start()
    get_basis.wait()
    basis = pair_rhs(basis_ref[...])
    starts, base, _ = gy_starts(sizes, patch)

    def row(i, carry):
        copy(i).wait()
        q0[i] = dot_nt(split_pairs(s_ref[i]), basis).astype(BF).reshape(patch // 2, VEC, 128)
        put_row(i).start()
        for half in range(2):
            cols = slice(half * 128, half * 128 + 128)
            gy_left[EDGE + base + 2 * i + half] = s_ref[i, 0, :, cols]
            gy_right[EDGE + base + 2 * i + half] = s_ref[i, patch - 1, :, cols]
        return carry

    lax.fori_loop(0, patch, row, 0)
    get_transfer.wait()
    for level in range(3):
        rhs = pair_rhs(transfer_ref[level])
        for r in range(sizes[level + 1]):
            qs[level + 1][r] = lift_rows(qs[level][2 * r], qs[level][2 * r + 1], rhs)
        put(level + 1).start()
    for number, unit in enumerate(gx_units(sizes, patch)):
        if unit[0] == "q":
            _, level, r, p = unit
            gx_lo[number] = qs[level][r, p]
            gx_hi[number] = qs[level][sizes[level] - 2 + r, p]
        else:
            _, cell, half = unit
            gx_lo[number] = s_ref[0, cell, :, half * 128 : half * 128 + 128]
            gx_hi[number] = s_ref[patch - 1, cell, :, half * 128 : half * 128 + 128]
    put(5).start()
    put(6).start()
    both = jnp.concatenate([q3[0, 0], q3[1, 0]], 1)
    both = jnp.concatenate([both[: VEC // 2], both[VEC // 2 :]], 1)
    top = dot_nt(both, pair_rhs(transfer_ref[3])).astype(BF)
    q4[...] = jnp.broadcast_to(top[None], q4.shape)
    put(4).start()
    zeros = jnp.zeros((EDGE, VEC, 128), BF)
    for ref in (gy_left, gy_right):
        ref[0:EDGE] = zeros
        ref[ref.shape[0] - EDGE : ref.shape[0]] = zeros
    for level in range(4):
        n = sizes[level]
        at = EDGE + starts[level]
        gy_left[at : at + n] = qs[level][:, 0]
        gy_right[at : at + n] = qs[level][:, n // 2 - 1]
    put(7).start()
    put(8).start()

    def wait_row(i, carry):
        put_row(i).wait()
        return carry

    lax.fori_loop(0, patch, wait_row, 0)
    for k in range(1, 9):
        put(k).wait()


def corner_kernel(from_lo, from_hi, left_in, right_in, left, right, buf, sems):
    del left_in, right_in
    n = left.shape[0]
    m = from_lo.shape[0]
    moves = [
        (from_lo.at[0:EDGE], left.at[0:EDGE]),
        (from_hi.at[0:EDGE], left.at[n - EDGE : n]),
        (from_lo.at[m - EDGE : m], right.at[0:EDGE]),
        (from_hi.at[m - EDGE : m], right.at[n - EDGE : n]),
    ]
    gets = [pltpu.make_async_copy(a, buf.at[k], sems.at[k]) for k, (a, b) in enumerate(moves)]
    puts = [pltpu.make_async_copy(buf.at[k], b, sems.at[4 + k]) for k, (a, b) in enumerate(moves)]
    for get in gets:
        get.start()
    for get, put in zip(gets, puts):
        get.wait()
        put.start()
    for put in puts:
        put.wait()


def list_words(codes, counts):
    slot = lax.broadcasted_iota(jnp.int32, codes.shape, codes.ndim - 1)
    active = slot < counts
    words = []
    for group in range(2):
        here = active & ((codes >= 18) if group else (codes < 18))
        shift = jnp.where(here, codes - 18 * group, 0)
        power = jnp.where(here, lax.shift_left(jnp.ones_like(codes), shift), 0)
        words.append(power.astype(F32))
    return words


def half_sizes(patch):
    return [patch // 2**k for k in range(4)]


def word_offsets(sizes):
    offsets = [0]
    for n in sizes:
        offsets.append(offsets[-1] + n * n)
    return offsets


def near_kernel(
    s_hbm, tiles_hbm, codes_hbm, counts_hbm, lo_hbm, hi_hbm, acc_hbm, words_hbm,
    s_ref, acc_ref, tiles_ref, words_ref, codes_ref, counts_ref, lo_ref, hi_ref,
    in_sems, out_sems, more_sems,
):
    patch = s_ref.shape[0]

    def fetch(i):
        return pltpu.make_async_copy(s_hbm.at[i], s_ref.at[i], in_sems.at[i])

    def put_out(k):
        rows = pl.ds(2 * k, 2)
        return pltpu.make_async_copy(acc_ref.at[rows], acc_hbm.at[rows], out_sems.at[k])

    def start_fetch(i, carry):
        fetch(i).start()
        return carry

    fetch_tiles = pltpu.make_async_copy(tiles_hbm, tiles_ref, more_sems.at[0])
    put_words = pltpu.make_async_copy(words_ref, words_hbm, more_sems.at[1])
    pairs = [(lo_hbm, lo_ref), (hi_hbm, hi_ref), (codes_hbm, codes_ref), (counts_hbm, counts_ref)]
    more = [pltpu.make_async_copy(a, b, more_sems.at[2 + k]) for k, (a, b) in enumerate(pairs)]
    more[0].start()
    fetch_tiles.start()
    lax.fori_loop(0, patch, start_fetch, 0)
    for copy in more[1:]:
        copy.start()
    fetch_tiles.wait()
    zeros = jnp.zeros((VEC, 256), BF)

    def shifted(value):
        return [
            jnp.concatenate([zeros, value[:-VEC]], 0),
            value,
            jnp.concatenate([value[VEC:], zeros], 0),
        ]

    def put(i, rows):
        blocks = [
            r if getattr(r, "ndim", 0) == 2 else s_ref[r].reshape(patch * VEC, 256) for r in rows
        ]
        lhs = []
        for d in range(3):
            for upper, lower in zip(shifted(blocks[d]), shifted(blocks[d + 1])):
                lhs.append(jnp.concatenate([upper, lower], 0))
        tiles = jnp.concatenate([tiles_ref[k] for k in range(9)], 1)
        out = dot_nt(jnp.concatenate(lhs, 1), tiles)
        acc_ref[pl.ds(i, 2)] = out.astype(BF).reshape(2, patch, VEC, 256)

    more[0].wait()
    for i in range(3):
        fetch(i).wait()
    cells = {unit[1:]: k for k, unit in enumerate(gx_units(half_sizes(patch), patch)) if unit[0] == "s"}

    def halo_row(ref):
        return jnp.concatenate(
            [
                jnp.concatenate([ref[cells[(j, half)]] for j in range(patch)], 0)
                for half in range(2)
            ],
            1,
        )

    put(0, [halo_row(lo_ref), 0, 1, 2])
    put_out(0).start()
    for copy in more[1:]:
        copy.wait()
    levels = counts_ref.shape[1]
    at = 0
    for level in range(levels):
        n = patch >> level
        counts = counts_ref[:, level : level + 1]
        codes = codes_ref[:, level, :]
        for group, power in enumerate(list_words(codes, counts)):
            word = jnp.sum(power, axis=1, keepdims=True).astype(jnp.int32)
            word = jnp.broadcast_to(word, (patch * patch, 128))
            if level == 0:
                words_ref[group, 0 : n * n] = word
                continue
            for i in range(n):
                for j in range(n):
                    r = (i * patch + j) << level
                    k = at + i * n + j
                    words_ref[group, k : k + 1] = word[r : r + 1]
        at += n * n
    put_words.start()

    def row(k, carry):
        i = 2 * k
        fetch(i + 1).wait()
        fetch(i + 2).wait()
        put(i, [i - 1, i, i + 1, i + 2])
        put_out(k).start()
        return carry

    lax.fori_loop(1, patch // 2 - 1, row, 0)
    fetch(patch - 1).wait()
    put(patch - 2, [patch - 3, patch - 2, patch - 1, halo_row(hi_ref)])
    put_out(patch // 2 - 1).start()

    def wait_out(k, carry):
        put_out(k).wait()
        return carry

    lax.fori_loop(0, patch // 2, wait_out, 0)
    put_words.wait()


def chunk_list(row_bit):
    chunks = []
    for a in range(6):
        for bp in range(3):
            if bp == 1 and 1 + row_bit <= a <= 3 + row_bit:
                continue
            chunks.append((a, bp))
    return chunks


def lane_bits():
    lane = lax.broadcasted_iota(jnp.int32, (8, 128), 1)
    return (lane >= 64).astype(jnp.int32)


def mask_of(words, a, bp, lanes):
    code = (a % 3) * 6 + 2 * bp
    bit = lax.shift_right_logical(words[a // 3], lanes + code) & 1
    m = bit.astype(F32)
    return jnp.concatenate([m, m, m, m], 0).astype(BF)


def upper_kernel(
    counts_upper_ref, codes_upper_ref, every_hbm, transfer_hbm, coupling_hbm, out_ref,
    every, transfer_ref, coupling_ref, shifted, f4, f5, f6, sems,
):
    pairs = [(every_hbm, every), (transfer_hbm, transfer_ref)]
    pairs += [(coupling_hbm.at[coupling_hbm.shape[0] - 1], coupling_ref)]
    copies = [pltpu.make_async_copy(a, b, sems.at[k]) for k, (a, b) in enumerate(pairs)]
    for copy in copies:
        copy.start()
    lanes = lane_bits()
    for copy in copies:
        copy.wait()
    for d in range(7):
        shifted[d] = coupling_ref[d, :, 64:448]

    f4[...] = jnp.zeros_like(f4)
    f5[...] = jnp.zeros_like(f5)
    f6[...] = jnp.zeros_like(f6)
    rows4 = f4.shape[0] - 4
    pairs4 = f4.shape[1] - 2
    low = lax.broadcasted_iota(jnp.int32, (pairs4, VEC // 2, 128), 2) < 64
    for r in range(rows4):
        v = every[2 * pairs4 * r : 2 * pairs4 * (r + 1)].astype(F32).reshape(pairs4, 2, VEC // 2, 128)
        even, odd = v[:, 0], v[:, 1]
        top = jnp.where(low, even, pltpu.roll(odd, 64, 2))
        bottom = jnp.where(low, pltpu.roll(even, 64, 2), odd)
        f4[r + 2, 1 : pairs4 + 1] = jnp.concatenate([top, bottom], 1).astype(BF)
    rhs4 = pair_rhs(transfer_ref[4])
    for child, parent in ((f4, f5), (f5, f6)):
        n_rows = parent.shape[0] - 4
        n_pairs = child.shape[1] - 2
        for r in range(n_rows):
            parent[r + 2, 1 : n_pairs // 2 + 1] = lift_rows(
                child[2 * r + 2, 1 : n_pairs + 1], child[2 * r + 3, 1 : n_pairs + 1], rhs4
            )
    row_index = lax.axis_index("gx")
    col_index = lax.axis_index("gy")
    upper_codes = codes_upper_ref[...]
    upper_slot = lax.broadcasted_iota(jnp.int32, upper_codes.shape, 0)
    upper_list = lax.broadcasted_iota(jnp.int32, upper_codes.shape, 1)

    def upper_words(index):
        count = jnp.where(upper_list == index, counts_upper_ref[index], 0)
        here = upper_slot < count
        words = []
        for group in range(2):
            mine = here & ((upper_codes >= 18) if group else (upper_codes < 18))
            shift = jnp.where(mine, upper_codes - 18 * group, 0)
            power = jnp.where(mine, lax.shift_left(jnp.ones_like(shift), shift), 0)
            total = jnp.sum(power.astype(F32), axis=0, keepdims=True)
            total = jnp.sum(total, axis=1, keepdims=True)
            words.append(jnp.broadcast_to(total, (8, 128)).astype(jnp.int32))
        return words

    uppers = []
    offset = 0
    for step, f in enumerate((f4, f5, f6)):
        r_here = lax.shift_right_logical(row_index, step)
        c_here = lax.shift_right_logical(col_index, step)
        n_cols = 2 * (f.shape[1] - 2)
        index = offset + r_here * n_cols + c_here
        offset += (f.shape[0] - 4) * n_cols
        words = upper_words(index)
        rb = r_here & 1
        cb = c_here & 1
        top_row = r_here - rb
        left = lax.shift_right_logical(c_here, 1)
        lhs, rhs = [], []
        for a in range(6):
            for bp in range(3):
                lhs.append(f[top_row + a, left + bp] * mask_of(words, a, bp, lanes))
            even = shifted[a + 1 - rb]
            odd = coupling_ref[a + 1 - rb][:, 0:384]
            rhs.append(jnp.where(cb == 1, odd, even))
        uppers.append(dot_nt(jnp.concatenate(lhs, 1), jnp.concatenate(rhs, 1)))
    down = uppers[-1]
    for step in (1, 0):
        r_here = lax.shift_right_logical(row_index, step)
        c_here = lax.shift_right_logical(col_index, step)
        carried = dot_nn(down.astype(BF), transfer_ref[4])
        half = jnp.where((r_here & 1) == 1, carried[:, 128:256], carried[:, 0:128])
        half = jnp.where((c_here & 1) == 1, pltpu.roll(half, 64, 1), half)
        down = uppers[step] + half[:, 0:64]
    out_ref[...] = dot_nn(down.astype(BF), transfer_ref[3])


def final_kernel(
    *refs,
):
    n_in = 14
    sources, coupling_hbm, out_ref = refs[:n_in], refs[n_in], refs[n_in + 1]
    buffers, rest = refs[n_in + 2 : 2 * n_in + 2], refs[2 * n_in + 2 :]
    (
        transfer_ref, carried_ref, words_ref, q0, q1, q2, q3,
        from_lo, from_hi, from_left, from_right, basis_ref, tiles_ref, acc_ref,
    ) = buffers
    (
    e0, e1, e2, e3, shifted, b0, b1, b2, b3, cols, edge_col, out_buf, coupling_ref,
    sems, in_sems, acc_sems, level_sems,
    ) = rest
    patch = acc_ref.shape[0]

    def fetch(k):
        return pltpu.make_async_copy(sources[k], buffers[k], in_sems.at[k])

    def fetch_acc(i):
        return pltpu.make_async_copy(sources[n_in - 1].at[i], acc_ref.at[i], acc_sems.at[i])

    def fetch_level(level):
        return pltpu.make_async_copy(
            coupling_hbm.at[level], coupling_ref.at[level], level_sems.at[level]
        )

    first = (9, 10, 12)
    for k in first:
        fetch(k).start()
    for k in range(n_in - 1):
        if k not in first:
            fetch(k).start()
    for level in (3, 2, 1, 0):
        fetch_level(level).start()

    def start_acc(i, carry):
        fetch_acc(i).start()
        return carry

    qs = [q0, q1, q2, q3]
    es = [e0, e1, e2, e3]
    sizes = [q.shape[0] for q in qs]
    lanes = lane_bits()
    word_at = word_offsets(sizes)

    def get_level(level):
        fetch_level(level).wait()
        for d in range(7):
            shifted[level, d] = coupling_ref[level, d, :, 64:448]

    def block(level, col_bit, d, bp):
        if col_bit == 1:
            return coupling_ref[level, d, :, bp * 128 : bp * 128 + 128]
        return shifted[level, d, :, bp * 128 : bp * 128 + 128]

    for k in first:
        fetch(k).wait()
    starts, base, total = gy_starts(sizes, patch)
    for side, ref in ((0, from_left), (1, from_right)):
        for half in range(2):
            c = slice(half * 128, half * 128 + 128)
            cols[side, 0, :, c] = ref[8 + half]
            cols[side, patch + 1, :, c] = ref[EDGE + total + 8 + half]
            for i in range(patch):
                cols[side, i + 1, :, c] = ref[EDGE + base + 2 * i + half]

    def images(level, group_rows, row_bit):
        n = sizes[level]
        e = es[level]
        out = []
        for col_bit in range(2):
            lhs, rhs = [], []
            words = []
            for group_row in group_rows:
                for group_col in range(n // 2):
                    at = word_at[level] + (2 * group_row + row_bit) * n + 2 * group_col + col_bit
                    words.append(
                        [
                            jnp.broadcast_to(words_ref[g, pl.ds(at, 1)], (8, 128))
                            for g in range(2)
                        ]
                    )
            for a, bp in chunk_list(row_bit):
                rows = []
                for number, pair in enumerate(words):
                    group_row = group_rows[number // (n // 2)]
                    group_col = number % (n // 2)
                    rows.append(
                        e[2 * group_row + a, group_col + bp] * mask_of(pair, a, bp, lanes)
                    )
                lhs.append(jnp.concatenate(rows, 0))
                rhs.append(block(level, col_bit, a + 1 - row_bit, bp))
            out.append(dot_nt(jnp.concatenate(lhs, 1), jnp.concatenate(rhs, 1)))
        return jnp.concatenate(out, 1)

    def spread_rhs(level):
        t = transfer_ref[level]
        z = jnp.zeros_like(t)
        return [jnp.concatenate([t, z], 0), jnp.concatenate([z, t], 0)]

    for side in range(2):
        lhs = jnp.concatenate(
            [cols[side, d : d + patch].reshape(patch * VEC, 256) for d in range(3)], 1
        )
        rhs = jnp.concatenate([tiles_ref[3 * d + 2 * side] for d in range(3)], 1)
        edge_col[side] = dot_nt(lhs, rhs).reshape(patch, VEC, 256)

    for k in range(n_in - 1):
        if k not in first:
            fetch(k).wait()
    for level in range(4):
        n = sizes[level]
        es[level][2 : n + 2, 1 : n // 2 + 1] = qs[level][...]
    for number, unit in enumerate(gx_units(sizes, patch)):
        if unit[0] == "q":
            _, level, r, p = unit
            es[level][r, p + 1] = from_lo[number]
            es[level][sizes[level] + 2 + r, p + 1] = from_hi[number]
    starts, base, total = gy_starts(sizes, patch)
    for side, ref in ((0, from_left), (1, from_right)):
        for level in range(4):
            n = sizes[level]
            p = 0 if side == 0 else n // 2 + 1
            es[level][0:2, p] = ref[2 * level : 2 * level + 2]
            es[level][2 : n + 2, p] = ref[EDGE + starts[level] : EDGE + starts[level] + n]
            hi = EDGE + total
            es[level][n + 2 : n + 4, p] = ref[hi + 2 * level : hi + 2 * level + 2]
    lax.fori_loop(0, patch, start_acc, 0)
    for level in (3, 2, 1, 0):
        get_level(level)
    carried3 = carried_ref[...]
    for row_bit in range(2):
        u = images(3, [0], row_bit)
        b3[row_bit, 0] = (u + carried3[:, row_bit * 128 : row_bit * 128 + 128]).astype(BF)

    def descend(level, parent, child, group_rows):
        n_pairs = parent.shape[1]
        count = len(group_rows)
        value = jnp.concatenate([parent[r].reshape(n_pairs * VEC, 128) for r in group_rows], 0)
        even, odd = [
            dot_nn(value, rhs).reshape(count, n_pairs, 1, VEC, 256) for rhs in spread_rhs(level)
        ]
        carried = jnp.concatenate([even, odd], 2).reshape(count, 2 * n_pairs, VEC, 256)
        for row_bit in range(2):
            u = images(level, group_rows, row_bit).reshape(count, 2 * n_pairs, VEC, 128)
            u = u + carried[:, :, :, row_bit * 128 : row_bit * 128 + 128]
            for number, group_row in enumerate(group_rows):
                child[2 * group_row + row_bit] = u[number].astype(BF)

    descend(2, b3, b2, [0, 1])
    descend(1, b2, b1, list(range(sizes[1] // 2)))

    basis = basis_ref[...]
    zb = jnp.zeros_like(basis)
    basis_pair = [jnp.concatenate([basis, zb], 0), jnp.concatenate([zb, basis], 0)]

    def copy(i):
        return pltpu.make_async_copy(out_buf.at[i], out_ref.at[i], sems.at[i])

    def finish(i, carry):
        fetch_acc(i).wait()
        value = b0[i].reshape(patch // 2 * VEC, 128)
        far = [dot_nn(value, rhs).reshape(patch // 2, 1, VEC, 256) for rhs in basis_pair]
        total_row = jnp.concatenate(far, 1).reshape(patch, VEC, 256) + acc_ref[i].astype(F32)
        first = total_row[0:1] + edge_col[0, pl.ds(i, 1)]
        last = total_row[patch - 1 : patch] + edge_col[1, pl.ds(i, 1)]
        total_row = jnp.concatenate([first, total_row[1 : patch - 1], last], 0)
        out_buf[i] = total_row.astype(BF)
        copy(i).start()
        return carry

    def loop0(k, carry):
        descend(0, b1, b0, [2 * k, 2 * k + 1])
        return lax.fori_loop(4 * k, 4 * k + 4, finish, carry)

    lax.fori_loop(0, sizes[0] // 4, loop0, 0)

    def loop_wait(i, carry):
        copy(i).wait()
        return carry

    lax.fori_loop(0, patch, loop_wait, 0)


def vspec():
    return pl.BlockSpec(memory_space=VMEM)


def sspec():
    return pl.BlockSpec(memory_space=pltpu.SMEM)


def shards(
    samples, leaf_basis, transfer, coupling, near_tiles,
    codes_local, counts_local, codes_upper, counts_upper,
):
    patch = samples.shape[0]
    sizes = [patch // 2**k for k in range(4)]
    n_gx = lax.axis_size("gx")
    n_gy = lax.axis_size("gy")
    units_gx = len(gx_units(sizes, patch))
    units_gy = gy_starts(sizes, patch)[2]
    params = pltpu.CompilerParams(vmem_limit_bytes=56 * 1024 * 1024)

    anywhere = pl.BlockSpec(memory_space=pl.ANY)
    shapes = [(n, n // 2, VEC, 128) for n in sizes]
    shapes += [(n_gx * n_gy, VEC // 2, 128)]
    shapes += [(units_gx, VEC, 128)] * 2 + [(units_gy + 2 * EDGE, VEC, 128)] * 2
    outs = pl.pallas_call(
        project_kernel,
        out_shape=[jax.ShapeDtypeStruct(v, BF) for v in shapes],
        in_specs=[anywhere] * 3,
        out_specs=[anywhere] * 9,
        scratch_shapes=[pltpu.VMEM(v, BF) for v in shapes]
        + [
            pltpu.VMEM((patch, patch, VEC, 256), BF),
            pltpu.VMEM(leaf_basis.shape, BF),
            pltpu.VMEM(transfer.shape, BF),
            pltpu.SemaphoreType.DMA((patch,)),
            pltpu.SemaphoreType.DMA((patch,)),
            pltpu.SemaphoreType.DMA((9,)),
            pltpu.SemaphoreType.DMA((2,)),
        ],
        compiler_params=params,
        name="project",
    )(samples, leaf_basis, transfer)
    q0, q1, q2, q3, q4, gx_lo, gx_hi, gy_left, gy_right = outs

    up = lambda n: [(i, i + 1) for i in range(n - 1)]
    dn = lambda n: [(i + 1, i) for i in range(n - 1)]
    from_lo = lax.ppermute(gx_hi, "gx", up(n_gx))
    from_hi = lax.ppermute(gx_lo, "gx", dn(n_gx))
    every = lax.all_to_all(q4, ("gx", "gy"), 0, 0, tiled=True)
    full = jax.ShapeDtypeStruct((units_gy + 2 * EDGE, VEC, 128), BF)
    send_left, send_right = pl.pallas_call(
        corner_kernel,
        out_shape=[full, full],
        in_specs=[anywhere] * 4,
        out_specs=[anywhere] * 2,
        scratch_shapes=[pltpu.VMEM((4, EDGE, VEC, 128), BF), pltpu.SemaphoreType.DMA((8,))],
        input_output_aliases={2: 0, 3: 1},
        compiler_params=params,
        name="corner",
    )(from_lo, from_hi, gy_left, gy_right)
    from_left = lax.ppermute(send_right, "gy", up(n_gy))
    from_right = lax.ppermute(send_left, "gy", dn(n_gy))

    n_words = -(-word_offsets(sizes)[-1] // 8) * 8
    codes = codes_local.reshape(patch * patch, *codes_local.shape[2:])
    counts = counts_local.reshape(patch * patch, counts_local.shape[2])
    acc, words = pl.pallas_call(
        near_kernel,
        out_shape=[
            jax.ShapeDtypeStruct((patch, patch, VEC, 256), BF),
            jax.ShapeDtypeStruct((2, n_words, 128), jnp.int32),
        ],
        in_specs=[anywhere] * 6,
        out_specs=[anywhere, anywhere],
        scratch_shapes=[
            pltpu.VMEM((patch, patch, VEC, 256), BF),
            pltpu.VMEM((patch, patch, VEC, 256), BF),
            pltpu.VMEM(near_tiles.shape, BF),
            pltpu.VMEM((2, n_words, 128), jnp.int32),
            pltpu.VMEM(codes.shape, codes.dtype),
            pltpu.VMEM(counts.shape, counts.dtype),
            pltpu.VMEM(from_lo.shape, BF),
            pltpu.VMEM(from_hi.shape, BF),
            pltpu.SemaphoreType.DMA((patch,)),
            pltpu.SemaphoreType.DMA((patch // 2,)),
            pltpu.SemaphoreType.DMA((6,)),
        ],
        compiler_params=params,
        name="near",
    )(
        samples, near_tiles, codes, counts, from_lo, from_hi,
    )

    def padded(rows, pairs):
        return pltpu.VMEM((rows + 4, pairs + 2, VEC, 128), BF)

    carried = pl.pallas_call(
        upper_kernel,
        out_shape=jax.ShapeDtypeStruct((VEC, transfer.shape[2]), F32),
        in_specs=[sspec(), vspec()] + [anywhere] * 3,
        out_specs=vspec(),
        scratch_shapes=[
            pltpu.VMEM(every.shape, BF),
            pltpu.VMEM(transfer.shape, BF),
            pltpu.VMEM(coupling.shape[1:], BF),
            pltpu.VMEM((7, RANK, 384), BF),
        ]
        + [padded(n_gx // 2**k, n_gy // 2 ** (k + 1)) for k in range(3)]
        + [pltpu.SemaphoreType.DMA((3,))],
        compiler_params=params,
        name="upper",
    )(counts_upper, codes_upper.T, every, transfer, coupling)
    inputs = [
        transfer, carried, words, q0, q1, q2, q3,
        from_lo, from_hi, from_left, from_right, leaf_basis, near_tiles, acc,
    ]
    scratch = [pltpu.VMEM(v.shape, v.dtype) for v in inputs]
    scratch += [padded(n, n // 2) for n in sizes]
    scratch += [pltpu.VMEM((4, 7, RANK, 384), BF)]
    scratch += [pltpu.VMEM((n, n // 2, VEC, 128), BF) for n in sizes]
    scratch += [
        pltpu.VMEM((2, patch + 2, VEC, 256), BF),
        pltpu.VMEM((2, patch, VEC, 256), F32),
        pltpu.VMEM((patch, patch, VEC, 256), BF),
        pltpu.VMEM((4, *coupling.shape[1:]), BF),
        pltpu.SemaphoreType.DMA((patch,)),
        pltpu.SemaphoreType.DMA((len(inputs) - 1,)),
        pltpu.SemaphoreType.DMA((patch,)),
        pltpu.SemaphoreType.DMA((4,)),
    ]
    return pl.pallas_call(
        final_kernel,
        out_shape=jax.ShapeDtypeStruct((patch, patch, VEC, 256), BF),
        in_specs=[anywhere] * (len(inputs) + 1),
        out_specs=pl.BlockSpec(memory_space=pl.ANY),
        scratch_shapes=scratch,
        compiler_params=params,
        name="final",
    )(
        *inputs, coupling,
    )


def solution(mesh):
    big = P("gx", "gy", None, None)
    in_specs = (big, P(), P(), P(), P(), big, P("gx", "gy", None), P(), P())
    return jax.shard_map(shards, mesh=mesh, in_specs=in_specs, out_specs=big, check_vma=False)
```

```python
import jax
import jax.numpy as jnp
from jax import lax
from jax.experimental import pallas as pl
from jax.experimental.pallas import tpu as pltpu
from jax.sharding import PartitionSpec as P


BF = jnp.bfloat16
F32 = jnp.float32
RANK = 64
VEC = 32
VMEM = pltpu.VMEM


def dot_nt(a, b):
    return lax.dot_general(a, b, (((1,), (1,)), ((), ())), preferred_element_type=F32)


def dot_nn(a, b):
    return lax.dot_general(a, b, (((1,), (0,)), ((), ())), preferred_element_type=F32)


def pair_rhs(matrix):
    zeros = jnp.zeros_like(matrix)
    return jnp.concatenate(
        [jnp.concatenate([matrix, zeros], 0), jnp.concatenate([zeros, matrix], 0)], 1
    )


def split_pairs(value):
    n, vec, k = value.shape
    v = value.reshape(n // 2, 2, vec, k)
    return jnp.concatenate(
        [v[:, 0].reshape(n // 2 * vec, k), v[:, 1].reshape(n // 2 * vec, k)], 1
    )


def lift_rows(upper, lower, rhs):
    both = jnp.concatenate([upper, lower], 2)
    out = dot_nt(split_pairs(both), rhs)
    return out.astype(BF).reshape(upper.shape[0] // 2, VEC, 128)


EDGE = 10


def gx_units(q_sizes, patch):
    def edge(last):
        units = []
        for level, n in enumerate(q_sizes):
            for row in range(2):
                units.append(("q", level, row, (n // 2 - 1) if last else 0))
        for half in range(2):
            units.append(("s", patch - 1 if last else 0, half))
        return units

    left, right = edge(False), edge(True)
    middle = []
    for level, n in enumerate(q_sizes):
        for row in range(2):
            for p in range(1, n // 2 - 1):
                middle.append(("q", level, row, p))
    for cell in range(1, patch - 1):
        for half in range(2):
            middle.append(("s", cell, half))
    return left + middle + right


def gy_starts(q_sizes, patch):
    starts = []
    at = 0
    for n in q_sizes:
        starts.append(at)
        at += n
    return starts, at, at + 2 * patch


def project_kernel(hbm_ref, basis_hbm, transfer_hbm, *refs):
    outs, bufs = refs[:9], refs[9:18]
    s_ref, basis_ref, transfer_ref, sems, row_sems, out_sems, more_sems = refs[18:]
    q0, q1, q2, q3, q4, gx_lo, gx_hi, gy_left, gy_right = bufs
    patch = s_ref.shape[0]
    qs = [q0, q1, q2, q3]
    sizes = [q.shape[0] for q in qs]

    def copy(i):
        return pltpu.make_async_copy(hbm_ref.at[i], s_ref.at[i], sems.at[i])

    def put_row(i):
        return pltpu.make_async_copy(q0.at[i], outs[0].at[i], row_sems.at[i])

    def put(k):
        return pltpu.make_async_copy(bufs[k], outs[k], out_sems.at[k])

    def fetch(i, carry):
        copy(i).start()
        return carry

    get_basis = pltpu.make_async_copy(basis_hbm, basis_ref, more_sems.at[0])
    get_transfer = pltpu.make_async_copy(transfer_hbm, transfer_ref, more_sems.at[1])
    get_basis.start()
    lax.fori_loop(0, patch, fetch, 0)
    get_transfer.start()
    get_basis.wait()
    basis = pair_rhs(basis_ref[...])
    starts, base, _ = gy_starts(sizes, patch)

    def row(i, carry):
        copy(i).wait()
        q0[i] = dot_nt(split_pairs(s_ref[i]), basis).astype(BF).reshape(patch // 2, VEC, 128)
        put_row(i).start()
        for half in range(2):
            cols = slice(half * 128, half * 128 + 128)
            gy_left[EDGE + base + 2 * i + half] = s_ref[i, 0, :, cols]
            gy_right[EDGE + base + 2 * i + half] = s_ref[i, patch - 1, :, cols]
        return carry

    lax.fori_loop(0, patch, row, 0)
    get_transfer.wait()
    for level in range(3):
        rhs = pair_rhs(transfer_ref[level])
        for r in range(sizes[level + 1]):
            qs[level + 1][r] = lift_rows(qs[level][2 * r], qs[level][2 * r + 1], rhs)
        put(level + 1).start()
    for number, unit in enumerate(gx_units(sizes, patch)):
        if unit[0] == "q":
            _, level, r, p = unit
            gx_lo[number] = qs[level][r, p]
            gx_hi[number] = qs[level][sizes[level] - 2 + r, p]
        else:
            _, cell, half = unit
            gx_lo[number] = s_ref[0, cell, :, half * 128 : half * 128 + 128]
            gx_hi[number] = s_ref[patch - 1, cell, :, half * 128 : half * 128 + 128]
    put(5).start()
    put(6).start()
    both = jnp.concatenate([q3[0, 0], q3[1, 0]], 1)
    both = jnp.concatenate([both[: VEC // 2], both[VEC // 2 :]], 1)
    top = dot_nt(both, pair_rhs(transfer_ref[3])).astype(BF)
    q4[...] = jnp.broadcast_to(top[None], q4.shape)
    put(4).start()
    zeros = jnp.zeros((EDGE, VEC, 128), BF)
    for ref in (gy_left, gy_right):
        ref[0:EDGE] = zeros
        ref[ref.shape[0] - EDGE : ref.shape[0]] = zeros
    for level in range(4):
        n = sizes[level]
        at = EDGE + starts[level]
        gy_left[at : at + n] = qs[level][:, 0]
        gy_right[at : at + n] = qs[level][:, n // 2 - 1]
    put(7).start()
    put(8).start()

    def wait_row(i, carry):
        put_row(i).wait()
        return carry

    lax.fori_loop(0, patch, wait_row, 0)
    for k in range(1, 9):
        put(k).wait()


def corner_kernel(from_lo, from_hi, left_in, right_in, left, right, buf, sems):
    del left_in, right_in
    n = left.shape[0]
    m = from_lo.shape[0]
    moves = [
        (from_lo.at[0:EDGE], left.at[0:EDGE]),
        (from_hi.at[0:EDGE], left.at[n - EDGE : n]),
        (from_lo.at[m - EDGE : m], right.at[0:EDGE]),
        (from_hi.at[m - EDGE : m], right.at[n - EDGE : n]),
    ]
    gets = [pltpu.make_async_copy(a, buf.at[k], sems.at[k]) for k, (a, b) in enumerate(moves)]
    puts = [pltpu.make_async_copy(buf.at[k], b, sems.at[4 + k]) for k, (a, b) in enumerate(moves)]
    for get in gets:
        get.start()
    for get, put in zip(gets, puts):
        get.wait()
        put.start()
    for put in puts:
        put.wait()


def list_words(codes, counts):
    slot = lax.broadcasted_iota(jnp.int32, codes.shape, codes.ndim - 1)
    active = slot < counts
    words = []
    for group in range(2):
        here = active & ((codes >= 18) if group else (codes < 18))
        shift = jnp.where(here, codes - 18 * group, 0)
        power = jnp.where(here, lax.shift_left(jnp.ones_like(codes), shift), 0)
        words.append(power.astype(F32))
    return words


def column(table):
    n, m = table.shape
    wide = jnp.broadcast_to(table[:, None, :], (n, m, m))
    row = lax.broadcasted_iota(jnp.int32, (n, m, m), 1)
    lane = lax.broadcasted_iota(jnp.int32, (n, m, m), 2)
    picked = jnp.where(row == lane, wide, 0).astype(F32)
    return jnp.sum(picked.reshape(n * m, m), axis=1, keepdims=True).astype(jnp.int32)


def half_sizes(patch):
    return [patch // 2**k for k in range(4)]


def word_offsets(sizes):
    offsets = [0]
    for n in sizes:
        offsets.append(offsets[-1] + n * n)
    return offsets


def near_kernel(
    s_hbm, tiles_hbm, codes_hbm, counts_hbm, lo_hbm, hi_hbm, acc_hbm, words_hbm,
    s_ref, acc_ref, tiles_ref, words_ref, codes_ref, counts_ref, lo_ref, hi_ref,
    in_sems, out_sems, more_sems,
):
    patch = s_ref.shape[0]

    def fetch(i):
        return pltpu.make_async_copy(s_hbm.at[i], s_ref.at[i], in_sems.at[i])

    def put_out(k):
        rows = pl.ds(2 * k, 2)
        return pltpu.make_async_copy(acc_ref.at[rows], acc_hbm.at[rows], out_sems.at[k])

    def start_fetch(i, carry):
        fetch(i).start()
        return carry

    fetch_tiles = pltpu.make_async_copy(tiles_hbm, tiles_ref, more_sems.at[0])
    put_words = pltpu.make_async_copy(words_ref, words_hbm, more_sems.at[1])
    pairs = [(lo_hbm, lo_ref), (hi_hbm, hi_ref), (codes_hbm, codes_ref), (counts_hbm, counts_ref)]
    more = [pltpu.make_async_copy(a, b, more_sems.at[2 + k]) for k, (a, b) in enumerate(pairs)]
    more[0].start()
    fetch_tiles.start()
    lax.fori_loop(0, patch, start_fetch, 0)
    for copy in more[1:]:
        copy.start()
    fetch_tiles.wait()
    zeros = jnp.zeros((VEC, 256), BF)

    def shifted(value):
        return [
            jnp.concatenate([zeros, value[:-VEC]], 0),
            value,
            jnp.concatenate([value[VEC:], zeros], 0),
        ]

    def put(i, rows):
        blocks = [
            r if getattr(r, "ndim", 0) == 2 else s_ref[r].reshape(patch * VEC, 256) for r in rows
        ]
        lhs = []
        for d in range(3):
            for upper, lower in zip(shifted(blocks[d]), shifted(blocks[d + 1])):
                lhs.append(jnp.concatenate([upper, lower], 0))
        tiles = jnp.concatenate([tiles_ref[k] for k in range(9)], 1)
        out = dot_nt(jnp.concatenate(lhs, 1), tiles)
        acc_ref[pl.ds(i, 2)] = out.astype(BF).reshape(2, patch, VEC, 256)

    more[0].wait()
    for i in range(3):
        fetch(i).wait()
    cells = {unit[1:]: k for k, unit in enumerate(gx_units(half_sizes(patch), patch)) if unit[0] == "s"}

    def halo_row(ref):
        return jnp.concatenate(
            [
                jnp.concatenate([ref[cells[(j, half)]] for j in range(patch)], 0)
                for half in range(2)
            ],
            1,
        )

    put(0, [halo_row(lo_ref), 0, 1, 2])
    put_out(0).start()
    for copy in more[1:]:
        copy.wait()
    levels = counts_ref.shape[1]
    at = 0
    for level in range(levels):
        n = patch >> level
        counts = column(counts_ref[:, level, :])
        codes = codes_ref[:, level, :]
        for group, power in enumerate(list_words(codes, counts)):
            word = jnp.sum(power, axis=1, keepdims=True).astype(jnp.int32)
            word = jnp.broadcast_to(word, (patch * patch, 128))
            if level == 0:
                words_ref[group, 0 : n * n] = word
                continue
            for i in range(n):
                for j in range(n):
                    r = (i * patch + j) << level
                    k = at + i * n + j
                    words_ref[group, k : k + 1] = word[r : r + 1]
        at += n * n
    put_words.start()

    def row(k, carry):
        i = 2 * k
        fetch(i + 1).wait()
        fetch(i + 2).wait()
        put(i, [i - 1, i, i + 1, i + 2])
        put_out(k).start()
        return carry

    lax.fori_loop(1, patch // 2 - 1, row, 0)
    fetch(patch - 1).wait()
    put(patch - 2, [patch - 3, patch - 2, patch - 1, halo_row(hi_ref)])
    put_out(patch // 2 - 1).start()

    def wait_out(k, carry):
        put_out(k).wait()
        return carry

    lax.fori_loop(0, patch // 2, wait_out, 0)
    put_words.wait()


def chunk_list(row_bit):
    chunks = []
    for a in range(6):
        for bp in range(3):
            if bp == 1 and 1 + row_bit <= a <= 3 + row_bit:
                continue
            chunks.append((a, bp))
    return chunks


def lane_bits():
    lane = lax.broadcasted_iota(jnp.int32, (8, 128), 1)
    return (lane >= 64).astype(jnp.int32)


def mask_of(words, a, bp, lanes):
    code = (a % 3) * 6 + 2 * bp
    bit = lax.shift_right_logical(words[a // 3], lanes + code) & 1
    m = bit.astype(F32)
    return jnp.concatenate([m, m, m, m], 0).astype(BF)


def final_kernel(
    counts_upper_ref, codes_upper_ref, *refs,
):
    n_in = 14
    sources, coupling_hbm, out_ref = refs[:n_in], refs[n_in], refs[n_in + 1]
    buffers, rest = refs[n_in + 2 : 2 * n_in + 2], refs[2 * n_in + 2 :]
    (
        transfer_ref, every, words_ref, q0, q1, q2, q3,
        from_lo, from_hi, from_left, from_right, basis_ref, tiles_ref, acc_ref,
    ) = buffers
    (
    e0, e1, e2, e3, f4, f5, f6, shifted, b0, b1, b2, b3, cols, edge_col, out_buf, coupling_ref,
    sems, in_sems, acc_sems, level_sems,
    ) = rest
    patch = acc_ref.shape[0]

    def fetch(k):
        return pltpu.make_async_copy(sources[k], buffers[k], in_sems.at[k])

    def fetch_acc(i):
        return pltpu.make_async_copy(sources[n_in - 1].at[i], acc_ref.at[i], acc_sems.at[i])

    def fetch_level(level):
        return pltpu.make_async_copy(
            coupling_hbm.at[level], coupling_ref.at[level], level_sems.at[level]
        )

    first = (9, 10, 12)
    fetch(1).start()
    fetch(0).start()
    fetch_level(4).start()
    for k in first:
        fetch(k).start()
    for k in range(2, n_in - 1):
        if k not in first:
            fetch(k).start()
    for level in (3, 2, 1, 0):
        fetch_level(level).start()

    def start_acc(i, carry):
        fetch_acc(i).start()
        return carry

    qs = [q0, q1, q2, q3]
    es = [e0, e1, e2, e3]
    sizes = [q.shape[0] for q in qs]
    lanes = lane_bits()
    word_at = word_offsets(sizes)

    def get_level(level):
        fetch_level(level).wait()
        for d in range(7):
            shifted[level, d] = coupling_ref[level, d, :, 64:448]

    def block(level, col_bit, d, bp):
        if col_bit == 1:
            return coupling_ref[level, d, :, bp * 128 : bp * 128 + 128]
        return shifted[level, d, :, bp * 128 : bp * 128 + 128]

    fetch(0).wait()
    fetch(1).wait()
    get_level(4)
    f4[...] = jnp.zeros_like(f4)
    f5[...] = jnp.zeros_like(f5)
    f6[...] = jnp.zeros_like(f6)
    rows4 = f4.shape[0] - 4
    pairs4 = f4.shape[1] - 2
    low = lax.broadcasted_iota(jnp.int32, (pairs4, VEC // 2, 128), 2) < 64
    for r in range(rows4):
        v = every[2 * pairs4 * r : 2 * pairs4 * (r + 1)].astype(F32).reshape(pairs4, 2, VEC // 2, 128)
        even, odd = v[:, 0], v[:, 1]
        top = jnp.where(low, even, pltpu.roll(odd, 64, 2))
        bottom = jnp.where(low, pltpu.roll(even, 64, 2), odd)
        f4[r + 2, 1 : pairs4 + 1] = jnp.concatenate([top, bottom], 1).astype(BF)
    rhs4 = pair_rhs(transfer_ref[4])
    for child, parent in ((f4, f5), (f5, f6)):
        n_rows = parent.shape[0] - 4
        n_pairs = child.shape[1] - 2
        for r in range(n_rows):
            parent[r + 2, 1 : n_pairs // 2 + 1] = lift_rows(
                child[2 * r + 2, 1 : n_pairs + 1], child[2 * r + 3, 1 : n_pairs + 1], rhs4
            )
    row_index = lax.axis_index("gx")
    col_index = lax.axis_index("gy")
    upper_codes = codes_upper_ref[...]
    upper_slot = lax.broadcasted_iota(jnp.int32, upper_codes.shape, 0)
    upper_list = lax.broadcasted_iota(jnp.int32, upper_codes.shape, 1)

    def upper_words(index):
        count = jnp.where(upper_list == index, counts_upper_ref[index], 0)
        here = upper_slot < count
        words = []
        for group in range(2):
            mine = here & ((upper_codes >= 18) if group else (upper_codes < 18))
            shift = jnp.where(mine, upper_codes - 18 * group, 0)
            power = jnp.where(mine, lax.shift_left(jnp.ones_like(shift), shift), 0)
            total = jnp.sum(power.astype(F32), axis=0, keepdims=True)
            total = jnp.sum(total, axis=1, keepdims=True)
            words.append(jnp.broadcast_to(total, (8, 128)).astype(jnp.int32))
        return words

    uppers = []
    offset = 0
    for step, f in enumerate((f4, f5, f6)):
        r_here = lax.shift_right_logical(row_index, step)
        c_here = lax.shift_right_logical(col_index, step)
        n_cols = 2 * (f.shape[1] - 2)
        index = offset + r_here * n_cols + c_here
        offset += (f.shape[0] - 4) * n_cols
        words = upper_words(index)
        rb = r_here & 1
        cb = c_here & 1
        top_row = r_here - rb
        left = lax.shift_right_logical(c_here, 1)
        lhs, rhs = [], []
        for a in range(6):
            for bp in range(3):
                lhs.append(f[top_row + a, left + bp] * mask_of(words, a, bp, lanes))
            even = shifted[4, a + 1 - rb]
            odd = coupling_ref[4, a + 1 - rb][:, 0:384]
            rhs.append(jnp.where(cb == 1, odd, even))
        uppers.append(dot_nt(jnp.concatenate(lhs, 1), jnp.concatenate(rhs, 1)))
    down = uppers[-1]
    for step in (1, 0):
        r_here = lax.shift_right_logical(row_index, step)
        c_here = lax.shift_right_logical(col_index, step)
        carried = dot_nn(down.astype(BF), transfer_ref[4])
        half = jnp.where((r_here & 1) == 1, carried[:, 128:256], carried[:, 0:128])
        half = jnp.where((c_here & 1) == 1, pltpu.roll(half, 64, 1), half)
        down = uppers[step] + half[:, 0:64]
    carried3 = dot_nn(down.astype(BF), transfer_ref[3])

    for k in first:
        fetch(k).wait()
    starts, base, total = gy_starts(sizes, patch)
    for side, ref in ((0, from_left), (1, from_right)):
        for half in range(2):
            c = slice(half * 128, half * 128 + 128)
            cols[side, 0, :, c] = ref[8 + half]
            cols[side, patch + 1, :, c] = ref[EDGE + total + 8 + half]
            for i in range(patch):
                cols[side, i + 1, :, c] = ref[EDGE + base + 2 * i + half]

    def images(level, group_rows, row_bit):
        n = sizes[level]
        e = es[level]
        out = []
        for col_bit in range(2):
            lhs, rhs = [], []
            words = []
            for group_row in group_rows:
                for group_col in range(n // 2):
                    at = word_at[level] + (2 * group_row + row_bit) * n + 2 * group_col + col_bit
                    words.append(
                        [
                            jnp.broadcast_to(words_ref[g, pl.ds(at, 1)], (8, 128))
                            for g in range(2)
                        ]
                    )
            for a, bp in chunk_list(row_bit):
                rows = []
                for number, pair in enumerate(words):
                    group_row = group_rows[number // (n // 2)]
                    group_col = number % (n // 2)
                    rows.append(
                        e[2 * group_row + a, group_col + bp] * mask_of(pair, a, bp, lanes)
                    )
                lhs.append(jnp.concatenate(rows, 0))
                rhs.append(block(level, col_bit, a + 1 - row_bit, bp))
            out.append(dot_nt(jnp.concatenate(lhs, 1), jnp.concatenate(rhs, 1)))
        return jnp.concatenate(out, 1)

    def spread_rhs(level):
        t = transfer_ref[level]
        z = jnp.zeros_like(t)
        return [jnp.concatenate([t, z], 0), jnp.concatenate([z, t], 0)]

    for side in range(2):
        lhs = jnp.concatenate(
            [cols[side, d : d + patch].reshape(patch * VEC, 256) for d in range(3)], 1
        )
        rhs = jnp.concatenate([tiles_ref[3 * d + 2 * side] for d in range(3)], 1)
        edge_col[side] = dot_nt(lhs, rhs).reshape(patch, VEC, 256)

    for k in range(2, n_in - 1):
        if k not in first:
            fetch(k).wait()
    for level in range(4):
        n = sizes[level]
        es[level][2 : n + 2, 1 : n // 2 + 1] = qs[level][...]
    for number, unit in enumerate(gx_units(sizes, patch)):
        if unit[0] == "q":
            _, level, r, p = unit
            es[level][r, p + 1] = from_lo[number]
            es[level][sizes[level] + 2 + r, p + 1] = from_hi[number]
    starts, base, total = gy_starts(sizes, patch)
    for side, ref in ((0, from_left), (1, from_right)):
        for level in range(4):
            n = sizes[level]
            p = 0 if side == 0 else n // 2 + 1
            es[level][0:2, p] = ref[2 * level : 2 * level + 2]
            es[level][2 : n + 2, p] = ref[EDGE + starts[level] : EDGE + starts[level] + n]
            hi = EDGE + total
            es[level][n + 2 : n + 4, p] = ref[hi + 2 * level : hi + 2 * level + 2]
    lax.fori_loop(0, patch, start_acc, 0)
    for level in (3, 2, 1, 0):
        get_level(level)
    for row_bit in range(2):
        u = images(3, [0], row_bit)
        b3[row_bit, 0] = (u + carried3[:, row_bit * 128 : row_bit * 128 + 128]).astype(BF)

    def descend(level, parent, child, group_rows):
        n_pairs = parent.shape[1]
        count = len(group_rows)
        value = jnp.concatenate([parent[r].reshape(n_pairs * VEC, 128) for r in group_rows], 0)
        even, odd = [
            dot_nn(value, rhs).reshape(count, n_pairs, 1, VEC, 256) for rhs in spread_rhs(level)
        ]
        carried = jnp.concatenate([even, odd], 2).reshape(count, 2 * n_pairs, VEC, 256)
        for row_bit in range(2):
            u = images(level, group_rows, row_bit).reshape(count, 2 * n_pairs, VEC, 128)
            u = u + carried[:, :, :, row_bit * 128 : row_bit * 128 + 128]
            for number, group_row in enumerate(group_rows):
                child[2 * group_row + row_bit] = u[number].astype(BF)

    descend(2, b3, b2, [0, 1])
    descend(1, b2, b1, list(range(sizes[1] // 2)))

    basis = basis_ref[...]
    zb = jnp.zeros_like(basis)
    basis_pair = [jnp.concatenate([basis, zb], 0), jnp.concatenate([zb, basis], 0)]

    def copy(i):
        return pltpu.make_async_copy(out_buf.at[i], out_ref.at[i], sems.at[i])

    def finish(i, carry):
        fetch_acc(i).wait()
        value = b0[i].reshape(patch // 2 * VEC, 128)
        far = [dot_nn(value, rhs).reshape(patch // 2, 1, VEC, 256) for rhs in basis_pair]
        total_row = jnp.concatenate(far, 1).reshape(patch, VEC, 256) + acc_ref[i].astype(F32)
        first = total_row[0:1] + edge_col[0, pl.ds(i, 1)]
        last = total_row[patch - 1 : patch] + edge_col[1, pl.ds(i, 1)]
        total_row = jnp.concatenate([first, total_row[1 : patch - 1], last], 0)
        out_buf[i] = total_row.astype(BF)
        copy(i).start()
        return carry

    def loop0(k, carry):
        descend(0, b1, b0, [2 * k, 2 * k + 1])
        return lax.fori_loop(4 * k, 4 * k + 4, finish, carry)

    lax.fori_loop(0, sizes[0] // 4, loop0, 0)

    def loop_wait(i, carry):
        copy(i).wait()
        return carry

    lax.fori_loop(0, patch, loop_wait, 0)


def vspec():
    return pl.BlockSpec(memory_space=VMEM)


def sspec():
    return pl.BlockSpec(memory_space=pltpu.SMEM)


def shards(
    samples, leaf_basis, transfer, coupling, near_tiles,
    codes_local, counts_local, codes_upper, counts_upper,
):
    patch = samples.shape[0]
    sizes = [patch // 2**k for k in range(4)]
    n_gx = lax.axis_size("gx")
    n_gy = lax.axis_size("gy")
    units_gx = len(gx_units(sizes, patch))
    units_gy = gy_starts(sizes, patch)[2]
    params = pltpu.CompilerParams(vmem_limit_bytes=56 * 1024 * 1024)

    anywhere = pl.BlockSpec(memory_space=pl.ANY)
    shapes = [(n, n // 2, VEC, 128) for n in sizes]
    shapes += [(n_gx * n_gy, VEC // 2, 128)]
    shapes += [(units_gx, VEC, 128)] * 2 + [(units_gy + 2 * EDGE, VEC, 128)] * 2
    outs = pl.pallas_call(
        project_kernel,
        out_shape=[jax.ShapeDtypeStruct(v, BF) for v in shapes],
        in_specs=[anywhere] * 3,
        out_specs=[anywhere] * 9,
        scratch_shapes=[pltpu.VMEM(v, BF) for v in shapes]
        + [
            pltpu.VMEM((patch, patch, VEC, 256), BF),
            pltpu.VMEM(leaf_basis.shape, BF),
            pltpu.VMEM(transfer.shape, BF),
            pltpu.SemaphoreType.DMA((patch,)),
            pltpu.SemaphoreType.DMA((patch,)),
            pltpu.SemaphoreType.DMA((9,)),
            pltpu.SemaphoreType.DMA((2,)),
        ],
        compiler_params=params,
        name="project",
    )(samples, leaf_basis, transfer)
    q0, q1, q2, q3, q4, gx_lo, gx_hi, gy_left, gy_right = outs

    up = lambda n: [(i, i + 1) for i in range(n - 1)]
    dn = lambda n: [(i + 1, i) for i in range(n - 1)]
    from_lo = lax.ppermute(gx_hi, "gx", up(n_gx))
    from_hi = lax.ppermute(gx_lo, "gx", dn(n_gx))
    every = lax.all_to_all(q4, ("gx", "gy"), 0, 0, tiled=True)
    full = jax.ShapeDtypeStruct((units_gy + 2 * EDGE, VEC, 128), BF)
    send_left, send_right = pl.pallas_call(
        corner_kernel,
        out_shape=[full, full],
        in_specs=[anywhere] * 4,
        out_specs=[anywhere] * 2,
        scratch_shapes=[pltpu.VMEM((4, EDGE, VEC, 128), BF), pltpu.SemaphoreType.DMA((8,))],
        input_output_aliases={2: 0, 3: 1},
        compiler_params=params,
        name="corner",
    )(from_lo, from_hi, gy_left, gy_right)
    from_left = lax.ppermute(send_right, "gy", up(n_gy))
    from_right = lax.ppermute(send_left, "gy", dn(n_gy))

    n_words = -(-word_offsets(sizes)[-1] // 8) * 8
    codes = codes_local.reshape(patch * patch, *codes_local.shape[2:])
    counts = counts_local.transpose(0, 2, 1)
    acc, words = pl.pallas_call(
        near_kernel,
        out_shape=[
            jax.ShapeDtypeStruct((patch, patch, VEC, 256), BF),
            jax.ShapeDtypeStruct((2, n_words, 128), jnp.int32),
        ],
        in_specs=[anywhere] * 6,
        out_specs=[anywhere, anywhere],
        scratch_shapes=[
            pltpu.VMEM((patch, patch, VEC, 256), BF),
            pltpu.VMEM((patch, patch, VEC, 256), BF),
            pltpu.VMEM(near_tiles.shape, BF),
            pltpu.VMEM((2, n_words, 128), jnp.int32),
            pltpu.VMEM(codes.shape, codes.dtype),
            pltpu.VMEM(counts.shape, counts.dtype),
            pltpu.VMEM(from_lo.shape, BF),
            pltpu.VMEM(from_hi.shape, BF),
            pltpu.SemaphoreType.DMA((patch,)),
            pltpu.SemaphoreType.DMA((patch // 2,)),
            pltpu.SemaphoreType.DMA((6,)),
        ],
        compiler_params=params,
        name="near",
    )(
        samples, near_tiles, codes, counts, from_lo, from_hi,
    )

    def padded(rows, pairs):
        return pltpu.VMEM((rows + 4, pairs + 2, VEC, 128), BF)

    inputs = [
        transfer, every, words, q0, q1, q2, q3,
        from_lo, from_hi, from_left, from_right, leaf_basis, near_tiles, acc,
    ]
    scratch = [pltpu.VMEM(v.shape, v.dtype) for v in inputs]
    scratch += [padded(n, n // 2) for n in sizes]
    scratch += [padded(n_gx // 2**k, n_gy // 2 ** (k + 1)) for k in range(3)]
    scratch += [pltpu.VMEM((5, 7, RANK, 384), BF)]
    scratch += [pltpu.VMEM((n, n // 2, VEC, 128), BF) for n in sizes]
    scratch += [
        pltpu.VMEM((2, patch + 2, VEC, 256), BF),
        pltpu.VMEM((2, patch, VEC, 256), F32),
        pltpu.VMEM((patch, patch, VEC, 256), BF),
        pltpu.VMEM(coupling.shape, BF),
        pltpu.SemaphoreType.DMA((patch,)),
        pltpu.SemaphoreType.DMA((len(inputs) - 1,)),
        pltpu.SemaphoreType.DMA((patch,)),
        pltpu.SemaphoreType.DMA((5,)),
    ]
    return pl.pallas_call(
        final_kernel,
        out_shape=jax.ShapeDtypeStruct((patch, patch, VEC, 256), BF),
        in_specs=[sspec(), vspec()] + [anywhere] * (len(inputs) + 1),
        out_specs=pl.BlockSpec(memory_space=pl.ANY),
        scratch_shapes=scratch,
        compiler_params=params,
        name="final",
    )(
        counts_upper, codes_upper.T, *inputs, coupling,
    )


def solution(mesh):
    big = P("gx", "gy", None, None)
    in_specs = (big, P(), P(), P(), P(), big, P("gx", "gy", None), P(), P())
    return jax.shard_map(shards, mesh=mesh, in_specs=in_specs, out_specs=big, check_vma=False)
```

```python
import jax
import jax.numpy as jnp
from jax import lax
from jax.experimental import pallas as pl
from jax.experimental.pallas import tpu as pltpu
from jax.sharding import PartitionSpec as P


BF = jnp.bfloat16
F32 = jnp.float32
RANK = 64
VEC = 32


def dot_nt(a, b):
    return lax.dot_general(a, b, (((1,), (1,)), ((), ())), preferred_element_type=F32)


def dot_nn(a, b):
    return lax.dot_general(a, b, (((1,), (0,)), ((), ())), preferred_element_type=F32)


def pair_rhs(matrix):
    zeros = jnp.zeros_like(matrix)
    return jnp.concatenate(
        [jnp.concatenate([matrix, zeros], 0), jnp.concatenate([zeros, matrix], 0)], 1
    )


def split_pairs(value):
    n, vec, k = value.shape
    v = value.reshape(n // 2, 2, vec, k)
    return jnp.concatenate(
        [v[:, 0].reshape(n // 2 * vec, k), v[:, 1].reshape(n // 2 * vec, k)], 1
    )


def lift_rows(upper, lower, rhs):
    both = jnp.concatenate([upper, lower], 2)
    out = dot_nt(split_pairs(both), rhs)
    return out.astype(BF).reshape(upper.shape[0] // 2, VEC, 128)


EDGE = 10


def gx_units(q_sizes, patch):
    def edge(last):
        units = []
        for level, n in enumerate(q_sizes):
            for row in range(2):
                units.append(("q", level, row, (n // 2 - 1) if last else 0))
        for half in range(2):
            units.append(("s", patch - 1 if last else 0, half))
        return units

    left, right = edge(False), edge(True)
    middle = []
    for level, n in enumerate(q_sizes):
        for row in range(2):
            for p in range(1, n // 2 - 1):
                middle.append(("q", level, row, p))
    for cell in range(1, patch - 1):
        for half in range(2):
            middle.append(("s", cell, half))
    return left + middle + right


def gy_starts(q_sizes, patch):
    starts = []
    at = 0
    for n in q_sizes:
        starts.append(at)
        at += n
    return starts, at, at + 2 * patch


def project_kernel(hbm_ref, basis_hbm, transfer_hbm, *refs):
    outs, bufs = refs[:9], refs[9:18]
    s_ref, basis_ref, transfer_ref, sems, row_sems, out_sems, more_sems = refs[18:]
    q0, q1, q2, q3, q4, gx_lo, gx_hi, gy_left, gy_right = bufs
    patch = s_ref.shape[0]
    qs = [q0, q1, q2, q3]
    sizes = [q.shape[0] for q in qs]

    def copy(i):
        return pltpu.make_async_copy(hbm_ref.at[i], s_ref.at[i], sems.at[i])

    def put_row(i):
        return pltpu.make_async_copy(q0.at[i], outs[0].at[i], row_sems.at[i])

    def put(k):
        return pltpu.make_async_copy(bufs[k], outs[k], out_sems.at[k])

    def fetch(i, carry):
        copy(i).start()
        return carry

    get_basis = pltpu.make_async_copy(basis_hbm, basis_ref, more_sems.at[0])
    get_transfer = pltpu.make_async_copy(transfer_hbm, transfer_ref, more_sems.at[1])
    get_basis.start()
    lax.fori_loop(0, patch, fetch, 0)
    get_transfer.start()
    get_basis.wait()
    basis = pair_rhs(basis_ref[...])
    starts, base, _ = gy_starts(sizes, patch)

    def row(i, carry):
        copy(i).wait()
        q0[i] = dot_nt(split_pairs(s_ref[i]), basis).astype(BF).reshape(patch // 2, VEC, 128)
        put_row(i).start()
        for half in range(2):
            cols = slice(half * 128, half * 128 + 128)
            gy_left[EDGE + base + 2 * i + half] = s_ref[i, 0, :, cols]
            gy_right[EDGE + base + 2 * i + half] = s_ref[i, patch - 1, :, cols]
        return carry

    lax.fori_loop(0, patch, row, 0)
    get_transfer.wait()
    for level in range(3):
        rhs = pair_rhs(transfer_ref[level])
        for r in range(sizes[level + 1]):
            qs[level + 1][r] = lift_rows(qs[level][2 * r], qs[level][2 * r + 1], rhs)
        put(level + 1).start()
    for number, unit in enumerate(gx_units(sizes, patch)):
        if unit[0] == "q":
            _, level, r, p = unit
            gx_lo[number] = qs[level][r, p]
            gx_hi[number] = qs[level][sizes[level] - 2 + r, p]
        else:
            _, cell, half = unit
            gx_lo[number] = s_ref[0, cell, :, half * 128 : half * 128 + 128]
            gx_hi[number] = s_ref[patch - 1, cell, :, half * 128 : half * 128 + 128]
    put(5).start()
    put(6).start()
    both = jnp.concatenate([q3[0, 0], q3[1, 0]], 1)
    both = jnp.concatenate([both[: VEC // 2], both[VEC // 2 :]], 1)
    top = dot_nt(both, pair_rhs(transfer_ref[3])).astype(BF)
    q4[...] = jnp.broadcast_to(top[None], q4.shape)
    put(4).start()
    zeros = jnp.zeros((EDGE, VEC, 128), BF)
    for ref in (gy_left, gy_right):
        ref[0:EDGE] = zeros
        ref[ref.shape[0] - EDGE : ref.shape[0]] = zeros
    for level in range(4):
        n = sizes[level]
        at = EDGE + starts[level]
        gy_left[at : at + n] = qs[level][:, 0]
        gy_right[at : at + n] = qs[level][:, n // 2 - 1]
    put(7).start()
    put(8).start()

    def wait_row(i, carry):
        put_row(i).wait()
        return carry

    lax.fori_loop(0, patch, wait_row, 0)
    for k in range(1, 9):
        put(k).wait()


def corner_kernel(from_lo, from_hi, left_in, right_in, left, right, buf, sems):
    del left_in, right_in
    n = left.shape[0]
    m = from_lo.shape[0]
    moves = [
        (from_lo.at[0:EDGE], left.at[0:EDGE]),
        (from_hi.at[0:EDGE], left.at[n - EDGE : n]),
        (from_lo.at[m - EDGE : m], right.at[0:EDGE]),
        (from_hi.at[m - EDGE : m], right.at[n - EDGE : n]),
    ]
    gets = [pltpu.make_async_copy(a, buf.at[k], sems.at[k]) for k, (a, b) in enumerate(moves)]
    puts = [pltpu.make_async_copy(buf.at[k], b, sems.at[4 + k]) for k, (a, b) in enumerate(moves)]
    for get in gets:
        get.start()
    for get, put in zip(gets, puts):
        get.wait()
        put.start()
    for put in puts:
        put.wait()


def list_words(codes, counts):
    slot = lax.broadcasted_iota(jnp.int32, codes.shape, codes.ndim - 1)
    active = slot < counts
    words = []
    for group in range(2):
        here = active & ((codes >= 18) if group else (codes < 18))
        shift = jnp.where(here, codes - 18 * group, 0)
        power = jnp.where(here, lax.shift_left(jnp.ones_like(codes), shift), 0)
        words.append(power.astype(F32))
    return words


def column(table):
    n, m = table.shape
    wide = jnp.broadcast_to(table[:, None, :], (n, m, m))
    row = lax.broadcasted_iota(jnp.int32, (n, m, m), 1)
    lane = lax.broadcasted_iota(jnp.int32, (n, m, m), 2)
    picked = jnp.where(row == lane, wide, 0).astype(F32)
    return jnp.sum(picked.reshape(n * m, m), axis=1, keepdims=True).astype(jnp.int32)


def half_sizes(patch):
    return [patch // 2**k for k in range(4)]


def word_offsets(sizes):
    offsets = [0]
    for n in sizes:
        offsets.append(offsets[-1] + n * n)
    return offsets


def near_kernel(
    s_hbm, tiles_hbm, codes_hbm, counts_hbm, lo_hbm, hi_hbm, acc_hbm, words_hbm,
    s_ref, acc_ref, tiles_ref, words_ref, codes_ref, counts_ref, lo_ref, hi_ref,
    in_sems, out_sems, more_sems,
):
    patch = s_ref.shape[0]

    def fetch(i):
        return pltpu.make_async_copy(s_hbm.at[i], s_ref.at[i], in_sems.at[i])

    def put_out(k):
        rows = pl.ds(2 * k, 2)
        return pltpu.make_async_copy(acc_ref.at[rows], acc_hbm.at[rows], out_sems.at[k])

    def start_fetch(i, carry):
        fetch(i).start()
        return carry

    fetch_tiles = pltpu.make_async_copy(tiles_hbm, tiles_ref, more_sems.at[0])
    put_words = pltpu.make_async_copy(words_ref, words_hbm, more_sems.at[1])
    pairs = [(lo_hbm, lo_ref), (hi_hbm, hi_ref), (codes_hbm, codes_ref), (counts_hbm, counts_ref)]
    more = [pltpu.make_async_copy(a, b, more_sems.at[2 + k]) for k, (a, b) in enumerate(pairs)]
    more[0].start()
    fetch_tiles.start()
    lax.fori_loop(0, patch, start_fetch, 0)
    for copy in more[1:]:
        copy.start()
    fetch_tiles.wait()
    zeros = jnp.zeros((VEC, 256), BF)

    def shifted(value):
        return [
            jnp.concatenate([zeros, value[:-VEC]], 0),
            value,
            jnp.concatenate([value[VEC:], zeros], 0),
        ]

    def put(i, rows):
        blocks = [
            r if getattr(r, "ndim", 0) == 2 else s_ref[r].reshape(patch * VEC, 256) for r in rows
        ]
        lhs = []
        for d in range(3):
            for upper, lower in zip(shifted(blocks[d]), shifted(blocks[d + 1])):
                lhs.append(jnp.concatenate([upper, lower], 0))
        tiles = jnp.concatenate([tiles_ref[k] for k in range(9)], 1)
        out = dot_nt(jnp.concatenate(lhs, 1), tiles)
        acc_ref[pl.ds(i, 2)] = out.astype(BF).reshape(2, patch, VEC, 256)

    more[0].wait()
    for i in range(3):
        fetch(i).wait()
    cells = {unit[1:]: k for k, unit in enumerate(gx_units(half_sizes(patch), patch)) if unit[0] == "s"}

    def halo_row(ref):
        return jnp.concatenate(
            [
                jnp.concatenate([ref[cells[(j, half)]] for j in range(patch)], 0)
                for half in range(2)
            ],
            1,
        )

    put(0, [halo_row(lo_ref), 0, 1, 2])
    put_out(0).start()
    for copy in more[1:]:
        copy.wait()
    levels = counts_ref.shape[1]
    at = 0
    for level in range(levels):
        n = patch >> level
        counts = column(counts_ref[:, level, :])
        codes = codes_ref[:, level, :]
        for group, power in enumerate(list_words(codes, counts)):
            word = jnp.sum(power, axis=1, keepdims=True).astype(jnp.int32)
            word = jnp.broadcast_to(word, (patch * patch, 128))
            if level == 0:
                words_ref[group, 0 : n * n] = word
                continue
            for i in range(n):
                for j in range(n):
                    r = (i * patch + j) << level
                    k = at + i * n + j
                    words_ref[group, k : k + 1] = word[r : r + 1]
        at += n * n
    put_words.start()

    def row(k, carry):
        i = 2 * k
        fetch(i + 1).wait()
        fetch(i + 2).wait()
        put(i, [i - 1, i, i + 1, i + 2])
        put_out(k).start()
        return carry

    lax.fori_loop(1, patch // 2 - 1, row, 0)
    fetch(patch - 1).wait()
    put(patch - 2, [patch - 3, patch - 2, patch - 1, halo_row(hi_ref)])
    put_out(patch // 2 - 1).start()

    def wait_out(k, carry):
        put_out(k).wait()
        return carry

    lax.fori_loop(0, patch // 2, wait_out, 0)
    put_words.wait()


def chunk_list(row_bit):
    chunks = []
    for a in range(6):
        for bp in range(3):
            if bp == 1 and 1 + row_bit <= a <= 3 + row_bit:
                continue
            chunks.append((a, bp))
    return chunks


def lane_bits():
    lane = lax.broadcasted_iota(jnp.int32, (8, 128), 1)
    return (lane >= 64).astype(jnp.int32)


def mask_of(words, a, bp, lanes):
    code = (a % 3) * 6 + 2 * bp
    bit = lax.shift_right_logical(words[a // 3], lanes + code) & 1
    m = bit.astype(F32)
    return jnp.concatenate([m, m, m, m], 0).astype(BF)


def final_kernel(
    counts_hbm, codes_hbm, *refs,
):
    n_in = 14
    sources, coupling_hbm, out_ref = refs[:n_in], refs[n_in], refs[n_in + 1]
    buffers, rest = refs[n_in + 2 : 2 * n_in + 2], refs[2 * n_in + 2 :]
    (
        transfer_ref, every, words_ref, q0, q1, q2, q3,
        from_lo, from_hi, from_left, from_right, basis_ref, tiles_ref, acc_ref,
    ) = buffers
    (
    e0, e1, e2, e3, f4, f5, f6, shifted, b0, b1, b2, b3, cols, edge_col, out_buf, coupling_ref,
    sems, in_sems, acc_sems, level_sems, counts_upper_ref, codes_upper_ref, list_sems,
    ) = rest
    patch = acc_ref.shape[0]

    def fetch(k):
        return pltpu.make_async_copy(sources[k], buffers[k], in_sems.at[k])

    def fetch_acc(i):
        return pltpu.make_async_copy(sources[n_in - 1].at[i], acc_ref.at[i], acc_sems.at[i])

    def fetch_level(level):
        return pltpu.make_async_copy(
            coupling_hbm.at[level], coupling_ref.at[level], level_sems.at[level]
        )

    first = (9, 10, 12)
    lists = [
        pltpu.make_async_copy(counts_hbm, counts_upper_ref, list_sems.at[0]),
        pltpu.make_async_copy(codes_hbm, codes_upper_ref, list_sems.at[1]),
    ]
    for copy_list in lists:
        copy_list.start()
    fetch(1).start()
    fetch(0).start()
    fetch_level(4).start()
    for k in first:
        fetch(k).start()
    for k in range(2, n_in - 1):
        if k not in first:
            fetch(k).start()
    for level in (3, 2, 1, 0):
        fetch_level(level).start()

    def start_acc(i, carry):
        fetch_acc(i).start()
        return carry

    qs = [q0, q1, q2, q3]
    es = [e0, e1, e2, e3]
    sizes = [q.shape[0] for q in qs]
    lanes = lane_bits()
    word_at = word_offsets(sizes)

    def get_level(level):
        fetch_level(level).wait()
        for d in range(7):
            shifted[level, d] = coupling_ref[level, d, :, 64:448]

    def block(level, col_bit, d, bp):
        if col_bit == 1:
            return coupling_ref[level, d, :, bp * 128 : bp * 128 + 128]
        return shifted[level, d, :, bp * 128 : bp * 128 + 128]

    for copy_list in lists:
        copy_list.wait()
    fetch(0).wait()
    fetch(1).wait()
    get_level(4)
    f4[...] = jnp.zeros_like(f4)
    f5[...] = jnp.zeros_like(f5)
    f6[...] = jnp.zeros_like(f6)
    rows4 = f4.shape[0] - 4
    pairs4 = f4.shape[1] - 2
    low = lax.broadcasted_iota(jnp.int32, (pairs4, VEC // 2, 128), 2) < 64
    for r in range(rows4):
        v = every[2 * pairs4 * r : 2 * pairs4 * (r + 1)].astype(F32).reshape(pairs4, 2, VEC // 2, 128)
        even, odd = v[:, 0], v[:, 1]
        top = jnp.where(low, even, pltpu.roll(odd, 64, 2))
        bottom = jnp.where(low, pltpu.roll(even, 64, 2), odd)
        f4[r + 2, 1 : pairs4 + 1] = jnp.concatenate([top, bottom], 1).astype(BF)
    rhs4 = pair_rhs(transfer_ref[4])
    for child, parent in ((f4, f5), (f5, f6)):
        n_rows = parent.shape[0] - 4
        n_pairs = child.shape[1] - 2
        for r in range(n_rows):
            parent[r + 2, 1 : n_pairs // 2 + 1] = lift_rows(
                child[2 * r + 2, 1 : n_pairs + 1], child[2 * r + 3, 1 : n_pairs + 1], rhs4
            )
    row_index = lax.axis_index("gx")
    col_index = lax.axis_index("gy")
    upper_codes = codes_upper_ref[...]
    upper_slot = lax.broadcasted_iota(jnp.int32, upper_codes.shape, 0)
    upper_list = lax.broadcasted_iota(jnp.int32, upper_codes.shape, 1)

    def upper_words(index):
        count = jnp.where(upper_list == index, counts_upper_ref[index], 0)
        here = upper_slot < count
        words = []
        for group in range(2):
            mine = here & ((upper_codes >= 18) if group else (upper_codes < 18))
            shift = jnp.where(mine, upper_codes - 18 * group, 0)
            power = jnp.where(mine, lax.shift_left(jnp.ones_like(shift), shift), 0)
            total = jnp.sum(power.astype(F32), axis=0, keepdims=True)
            total = jnp.sum(total, axis=1, keepdims=True)
            words.append(jnp.broadcast_to(total, (8, 128)).astype(jnp.int32))
        return words

    uppers = []
    offset = 0
    for step, f in enumerate((f4, f5, f6)):
        r_here = lax.shift_right_logical(row_index, step)
        c_here = lax.shift_right_logical(col_index, step)
        n_cols = 2 * (f.shape[1] - 2)
        index = offset + r_here * n_cols + c_here
        offset += (f.shape[0] - 4) * n_cols
        words = upper_words(index)
        rb = r_here & 1
        cb = c_here & 1
        top_row = r_here - rb
        left = lax.shift_right_logical(c_here, 1)
        lhs, rhs = [], []
        for a in range(6):
            for bp in range(3):
                lhs.append(f[top_row + a, left + bp] * mask_of(words, a, bp, lanes))
            even = shifted[4, a + 1 - rb]
            odd = coupling_ref[4, a + 1 - rb][:, 0:384]
            rhs.append(jnp.where(cb == 1, odd, even))
        uppers.append(dot_nt(jnp.concatenate(lhs, 1), jnp.concatenate(rhs, 1)))
    down = uppers[-1]
    for step in (1, 0):
        r_here = lax.shift_right_logical(row_index, step)
        c_here = lax.shift_right_logical(col_index, step)
        carried = dot_nn(down.astype(BF), transfer_ref[4])
        half = jnp.where((r_here & 1) == 1, carried[:, 128:256], carried[:, 0:128])
        half = jnp.where((c_here & 1) == 1, pltpu.roll(half, 64, 1), half)
        down = uppers[step] + half[:, 0:64]
    carried3 = dot_nn(down.astype(BF), transfer_ref[3])

    for k in first:
        fetch(k).wait()
    starts, base, total = gy_starts(sizes, patch)
    for side, ref in ((0, from_left), (1, from_right)):
        for half in range(2):
            c = slice(half * 128, half * 128 + 128)
            cols[side, 0, :, c] = ref[8 + half]
            cols[side, patch + 1, :, c] = ref[EDGE + total + 8 + half]
            for i in range(patch):
                cols[side, i + 1, :, c] = ref[EDGE + base + 2 * i + half]

    def images(level, group_rows, row_bit):
        n = sizes[level]
        e = es[level]
        out = []
        for col_bit in range(2):
            lhs, rhs = [], []
            words = []
            for group_row in group_rows:
                for group_col in range(n // 2):
                    at = word_at[level] + (2 * group_row + row_bit) * n + 2 * group_col + col_bit
                    words.append(
                        [
                            jnp.broadcast_to(words_ref[g, pl.ds(at, 1)], (8, 128))
                            for g in range(2)
                        ]
                    )
            for a, bp in chunk_list(row_bit):
                rows = []
                for number, pair in enumerate(words):
                    group_row = group_rows[number // (n // 2)]
                    group_col = number % (n // 2)
                    rows.append(
                        e[2 * group_row + a, group_col + bp] * mask_of(pair, a, bp, lanes)
                    )
                lhs.append(jnp.concatenate(rows, 0))
                rhs.append(block(level, col_bit, a + 1 - row_bit, bp))
            out.append(dot_nt(jnp.concatenate(lhs, 1), jnp.concatenate(rhs, 1)))
        return jnp.concatenate(out, 1)

    def spread_rhs(level):
        t = transfer_ref[level]
        z = jnp.zeros_like(t)
        return [jnp.concatenate([t, z], 0), jnp.concatenate([z, t], 0)]

    for side in range(2):
        lhs = jnp.concatenate(
            [cols[side, d : d + patch].reshape(patch * VEC, 256) for d in range(3)], 1
        )
        rhs = jnp.concatenate([tiles_ref[3 * d + 2 * side] for d in range(3)], 1)
        edge_col[side] = dot_nt(lhs, rhs).reshape(patch, VEC, 256)

    for k in range(2, n_in - 1):
        if k not in first:
            fetch(k).wait()
    for level in range(4):
        n = sizes[level]
        es[level][2 : n + 2, 1 : n // 2 + 1] = qs[level][...]
    for number, unit in enumerate(gx_units(sizes, patch)):
        if unit[0] == "q":
            _, level, r, p = unit
            es[level][r, p + 1] = from_lo[number]
            es[level][sizes[level] + 2 + r, p + 1] = from_hi[number]
    starts, base, total = gy_starts(sizes, patch)
    for side, ref in ((0, from_left), (1, from_right)):
        for level in range(4):
            n = sizes[level]
            p = 0 if side == 0 else n // 2 + 1
            es[level][0:2, p] = ref[2 * level : 2 * level + 2]
            es[level][2 : n + 2, p] = ref[EDGE + starts[level] : EDGE + starts[level] + n]
            hi = EDGE + total
            es[level][n + 2 : n + 4, p] = ref[hi + 2 * level : hi + 2 * level + 2]
    lax.fori_loop(0, patch, start_acc, 0)
    for level in (3, 2, 1, 0):
        get_level(level)
    for row_bit in range(2):
        u = images(3, [0], row_bit)
        b3[row_bit, 0] = (u + carried3[:, row_bit * 128 : row_bit * 128 + 128]).astype(BF)

    def descend(level, parent, child, group_rows):
        n_pairs = parent.shape[1]
        count = len(group_rows)
        value = jnp.concatenate([parent[r].reshape(n_pairs * VEC, 128) for r in group_rows], 0)
        even, odd = [
            dot_nn(value, rhs).reshape(count, n_pairs, 1, VEC, 256) for rhs in spread_rhs(level)
        ]
        carried = jnp.concatenate([even, odd], 2).reshape(count, 2 * n_pairs, VEC, 256)
        for row_bit in range(2):
            u = images(level, group_rows, row_bit).reshape(count, 2 * n_pairs, VEC, 128)
            u = u + carried[:, :, :, row_bit * 128 : row_bit * 128 + 128]
            for number, group_row in enumerate(group_rows):
                child[2 * group_row + row_bit] = u[number].astype(BF)

    descend(2, b3, b2, [0, 1])
    descend(1, b2, b1, list(range(sizes[1] // 2)))

    basis = basis_ref[...]
    zb = jnp.zeros_like(basis)
    basis_pair = [jnp.concatenate([basis, zb], 0), jnp.concatenate([zb, basis], 0)]

    def copy(i):
        return pltpu.make_async_copy(out_buf.at[i], out_ref.at[i], sems.at[i])

    def finish(i, carry):
        fetch_acc(i).wait()
        value = b0[i].reshape(patch // 2 * VEC, 128)
        far = [dot_nn(value, rhs).reshape(patch // 2, 1, VEC, 256) for rhs in basis_pair]
        total_row = jnp.concatenate(far, 1).reshape(patch, VEC, 256) + acc_ref[i].astype(F32)
        first = total_row[0:1] + edge_col[0, pl.ds(i, 1)]
        last = total_row[patch - 1 : patch] + edge_col[1, pl.ds(i, 1)]
        total_row = jnp.concatenate([first, total_row[1 : patch - 1], last], 0)
        out_buf[i] = total_row.astype(BF)
        copy(i).start()
        return carry

    def loop0(k, carry):
        descend(0, b1, b0, [2 * k, 2 * k + 1])
        return lax.fori_loop(4 * k, 4 * k + 4, finish, carry)

    lax.fori_loop(0, sizes[0] // 4, loop0, 0)

    def loop_wait(i, carry):
        copy(i).wait()
        return carry

    lax.fori_loop(0, patch, loop_wait, 0)


def shards(
    samples, leaf_basis, transfer, coupling, near_tiles,
    codes_local, counts_local, codes_upper, counts_upper,
):
    patch = samples.shape[0]
    sizes = [patch // 2**k for k in range(4)]
    n_gx = lax.axis_size("gx")
    n_gy = lax.axis_size("gy")
    units_gx = len(gx_units(sizes, patch))
    units_gy = gy_starts(sizes, patch)[2]
    params = pltpu.CompilerParams(vmem_limit_bytes=56 * 1024 * 1024)

    anywhere = pl.BlockSpec(memory_space=pl.ANY)
    shapes = [(n, n // 2, VEC, 128) for n in sizes]
    shapes += [(n_gx * n_gy, VEC // 2, 128)]
    shapes += [(units_gx, VEC, 128)] * 2 + [(units_gy + 2 * EDGE, VEC, 128)] * 2
    outs = pl.pallas_call(
        project_kernel,
        out_shape=[jax.ShapeDtypeStruct(v, BF) for v in shapes],
        in_specs=[anywhere] * 3,
        out_specs=[anywhere] * 9,
        scratch_shapes=[pltpu.VMEM(v, BF) for v in shapes]
        + [
            pltpu.VMEM((patch, patch, VEC, 256), BF),
            pltpu.VMEM(leaf_basis.shape, BF),
            pltpu.VMEM(transfer.shape, BF),
            pltpu.SemaphoreType.DMA((patch,)),
            pltpu.SemaphoreType.DMA((patch,)),
            pltpu.SemaphoreType.DMA((9,)),
            pltpu.SemaphoreType.DMA((2,)),
        ],
        compiler_params=params,
        name="project",
    )(samples, leaf_basis, transfer)
    q0, q1, q2, q3, q4, gx_lo, gx_hi, gy_left, gy_right = outs

    up = lambda n: [(i, i + 1) for i in range(n - 1)]
    dn = lambda n: [(i + 1, i) for i in range(n - 1)]
    from_lo = lax.ppermute(gx_hi, "gx", up(n_gx))
    from_hi = lax.ppermute(gx_lo, "gx", dn(n_gx))
    every = lax.all_to_all(q4, ("gx", "gy"), 0, 0, tiled=True)
    full = jax.ShapeDtypeStruct((units_gy + 2 * EDGE, VEC, 128), BF)
    send_left, send_right = pl.pallas_call(
        corner_kernel,
        out_shape=[full, full],
        in_specs=[anywhere] * 4,
        out_specs=[anywhere] * 2,
        scratch_shapes=[pltpu.VMEM((4, EDGE, VEC, 128), BF), pltpu.SemaphoreType.DMA((8,))],
        input_output_aliases={2: 0, 3: 1},
        compiler_params=params,
        name="corner",
    )(from_lo, from_hi, gy_left, gy_right)
    from_left = lax.ppermute(send_right, "gy", up(n_gy))
    from_right = lax.ppermute(send_left, "gy", dn(n_gy))

    n_words = -(-word_offsets(sizes)[-1] // 8) * 8
    codes = codes_local.reshape(patch * patch, *codes_local.shape[2:])
    counts = counts_local.transpose(0, 2, 1)
    acc, words = pl.pallas_call(
        near_kernel,
        out_shape=[
            jax.ShapeDtypeStruct((patch, patch, VEC, 256), BF),
            jax.ShapeDtypeStruct((2, n_words, 128), jnp.int32),
        ],
        in_specs=[anywhere] * 6,
        out_specs=[anywhere, anywhere],
        scratch_shapes=[
            pltpu.VMEM((patch, patch, VEC, 256), BF),
            pltpu.VMEM((patch, patch, VEC, 256), BF),
            pltpu.VMEM(near_tiles.shape, BF),
            pltpu.VMEM((2, n_words, 128), jnp.int32),
            pltpu.VMEM(codes.shape, codes.dtype),
            pltpu.VMEM(counts.shape, counts.dtype),
            pltpu.VMEM(from_lo.shape, BF),
            pltpu.VMEM(from_hi.shape, BF),
            pltpu.SemaphoreType.DMA((patch,)),
            pltpu.SemaphoreType.DMA((patch // 2,)),
            pltpu.SemaphoreType.DMA((6,)),
        ],
        compiler_params=params,
        name="near",
    )(
        samples, near_tiles, codes, counts, from_lo, from_hi,
    )

    def padded(rows, pairs):
        return pltpu.VMEM((rows + 4, pairs + 2, VEC, 128), BF)

    inputs = [
        transfer, every, words, q0, q1, q2, q3,
        from_lo, from_hi, from_left, from_right, leaf_basis, near_tiles, acc,
    ]
    scratch = [pltpu.VMEM(v.shape, v.dtype) for v in inputs]
    scratch += [padded(n, n // 2) for n in sizes]
    scratch += [padded(n_gx // 2**k, n_gy // 2 ** (k + 1)) for k in range(3)]
    scratch += [pltpu.VMEM((5, 7, RANK, 384), BF)]
    scratch += [pltpu.VMEM((n, n // 2, VEC, 128), BF) for n in sizes]
    scratch += [
        pltpu.VMEM((2, patch + 2, VEC, 256), BF),
        pltpu.VMEM((2, patch, VEC, 256), F32),
        pltpu.VMEM((patch, patch, VEC, 256), BF),
        pltpu.VMEM(coupling.shape, BF),
        pltpu.SemaphoreType.DMA((patch,)),
        pltpu.SemaphoreType.DMA((len(inputs) - 1,)),
        pltpu.SemaphoreType.DMA((patch,)),
        pltpu.SemaphoreType.DMA((5,)),
        pltpu.SMEM(counts_upper.shape, jnp.int32),
        pltpu.VMEM(codes_upper.shape[::-1], jnp.int32),
        pltpu.SemaphoreType.DMA((2,)),
    ]
    return pl.pallas_call(
        final_kernel,
        out_shape=jax.ShapeDtypeStruct((patch, patch, VEC, 256), BF),
        in_specs=[anywhere] * (len(inputs) + 3),
        out_specs=pl.BlockSpec(memory_space=pl.ANY),
        scratch_shapes=scratch,
        compiler_params=params,
        name="final",
    )(
        counts_upper, codes_upper.T, *inputs, coupling,
    )


def solution(mesh):
    big = P("gx", "gy", None, None)
    in_specs = (big, P(), P(), P(), P(), big, P("gx", "gy", None), P(), P())
    return jax.shard_map(shards, mesh=mesh, in_specs=in_specs, out_specs=big, check_vma=False)
```
